512 devices in a mesh: seq: 128 (over z, x, core), ch: 4 (over y).
Axes of the slice: x: 4, y: 4, z: 16, core: 2. Of those that a mesh axis runs over, the one named last changes fastest.
Arguments:
- values: float32 [32768, 1024], P('seq', 'ch'), may hold values from -6 to 6
- gates: float32 [32768, 1024], P('seq', 'ch'), may hold values from -6 to 6
- filter_taps: float32 [4096, 1024], P('seq', 'ch'), may hold values from -0.09375 to 0.09375
- skip: float32 [1024], P('ch'), may hold values from 0.5 to 2
- out_weight: bfloat16 [1024, 2048], P(None, 'ch'), may hold values from -0.1875 to 0.1875
Outputs:
- mixed: float32 [32768, 2048], P('seq', 'ch')
The draws below stay inside these ranges and needn't reach their ends.
All inputs are finite; a program needn't handle non-finite values.
Results may differ from the reference program's by a relative error of at most 0.0058.
Values may be sent and summed in bfloat16 or wider, within the bound.
A program may use at most 64 MiB of HBM per device.

```python
import jax
import jax.numpy as jnp

D = 2048
CHANNELS = 1024
FILTER = 4096
TOKENS = 32768


def shard_levels(key, dims, shards, low, top_value):
    factor_of, own = 1.0, jax.random.fold_in(key, 6)
    for position, parts in shards:
        steps = jnp.exp(jax.random.uniform(jax.random.fold_in(own, position), (parts,), jnp.float32, low / len(shards), top_value / len(shards)))
        factor_of = factor_of * jnp.repeat(steps, dims[position] // parts).reshape([-1 if axis == position else 1 for axis in range(len(dims))])
    return factor_of


def gaussian(rng, shape, deviation, bound, split=(), kind=jnp.bfloat16):
    loudness = shard_levels(rng, shape, split, -0.22, 0.18) if split else 1.0
    result = jax.random.normal(rng, shape, jnp.float32) * deviation * loudness
    return jnp.minimum(jnp.maximum(result, -bound), bound).astype(kind)


def setup_inputs(seed: int = 0) -> dict:
    arg_keys = jax.random.split(jax.random.key(seed), 6)
    return {
        "values": gaussian(arg_keys[0], (TOKENS, CHANNELS), 1.0, 6.0, ((0, 128), (1, 4)), jnp.float32),
        "gates": gaussian(arg_keys[1], (TOKENS, CHANNELS), 1.0, 6.0, ((0, 128), (1, 4)), jnp.float32),
        "filter_taps": gaussian(arg_keys[2], (FILTER, CHANNELS), FILTER ** -0.5, 0.09375, ((0, 128), (1, 4)), jnp.float32),
        "skip": jnp.clip(0.5 + 1.5 * jax.random.uniform(arg_keys[3], (CHANNELS,), jnp.float32) ** shard_levels(arg_keys[3], (CHANNELS,), ((0, 4),), -0.2, 0.2), 0.5, 2.0),
        "out_weight": gaussian(arg_keys[4], (CHANNELS, D), CHANNELS ** -0.5, 0.1875, ((1, 4),)),
    }


def reference(values, gates, filter_taps, skip, out_weight):
    length = values.shape[0]
    padded = 1 << (length + FILTER - 1).bit_length()
    spectrum = jnp.fft.rfft(values, n=padded, axis=0) * jnp.fft.rfft(filter_taps, n=padded, axis=0)
    convolved = jnp.fft.irfft(spectrum, n=padded, axis=0)[:length]
    hidden = (gates * (convolved + skip[None, :] * values)).astype(jnp.bfloat16)
    return jnp.dot(hidden, out_weight, preferred_element_type=jnp.float32)
```

```python
import functools

import jax
import jax.numpy as jnp
from jax import lax
from jax.experimental import pallas as pl
from jax.experimental.pallas import tpu as pltpu
from jax.sharding import Mesh
from jax.sharding import PartitionSpec as P

MESH = pl.DeviceIdType.MESH
F32 = jnp.float32
BF16 = jnp.bfloat16
VMEM = pltpu.VMEM
ANY = pl.BlockSpec(memory_space=pl.ANY)
NZ, NW = 16, 8


def each(low, high, step):
    def run(k, _):
        step(k)
        return 0

    lax.fori_loop(low, high, run, 0)


def greet(axis, size):
    me = lax.axis_index(axis)
    barrier = pltpu.get_barrier_semaphore()
    for k in range(1, size):
        pl.semaphore_signal(barrier, inc=1, device_id={axis: lax.rem(me + k, size)}, device_id_type=MESH)


def wait_for(count):
    pl.semaphore_wait(pltpu.get_barrier_semaphore(), count)


def spread_kernel(values_hbm, taps_hbm, out, values, taps, send_values, send_taps, got_taps, local_sem, send_sem, recv_sem):
    me = lax.axis_index("w")
    greet("w", NW)
    loads = [
        pltpu.make_async_copy(taps_hbm, taps, local_sem.at[0]),
        pltpu.make_async_copy(values_hbm, values, local_sem.at[1]),
    ]
    for load in loads:
        load.start()
    loads[0].wait()
    own = jnp.concatenate([taps[...], jnp.zeros((96, 256), F32)], axis=0)
    own = pltpu.roll(own.T, 32 * lax.rem(me, 4), 1)
    send_taps[...] = own.astype(BF16).reshape(NW, NZ, 2, 128)
    loads[1].wait()
    for half in range(2):
        turned = values[half * 128:(half + 1) * 128, :].T
        send_values[half] = turned.astype(BF16).reshape(NW, NZ, 2, 128)
    wait_for(NW - 1)

    def taps_to(k):
        peer = lax.rem(me + k, NW)
        return pltpu.make_async_remote_copy(
            src_ref=send_taps.at[peer], dst_ref=got_taps.at[k], send_sem=send_sem.at[0, k],
            recv_sem=recv_sem.at[0, k], device_id={"w": peer}, device_id_type=MESH)

    def values_to(k):
        peer = lax.rem(me + k, NW)
        return pltpu.make_async_remote_copy(
            src_ref=send_values.at[:, peer], dst_ref=out.at[pl.ds(2 * me, 2)], send_sem=send_sem.at[1, k],
            recv_sem=recv_sem.at[1, k], device_id={"w": peer}, device_id_type=MESH)

    order = (4, 3, 5, 2, 6, 1, 7)
    for k in order:
        taps_to(k).start()
        values_to(k).start()
    out[pl.ds(2 * me, 2)] = send_values[:, me]
    got_taps[0] = send_taps[me]
    for k in order:
        taps_to(k).wait()
    for half in range(2):
        from_w = lambda w: got_taps[lax.rem(me + NW - w, NW)]
        w = 4 * half
        out[16 + half] = (from_w(w) + from_w(w + 1)) + (from_w(w + 2) + from_w(w + 3))
    for k in order:
        values_to(k).wait()


def convolve_kernel(rows_hbm, back, rows, got, got_taps, blocks, lags, toeplitz, total, results, local_sem, send_sem, recv_sem):
    me = lax.axis_index("z")
    greet("z", NZ)
    load = pltpu.make_async_copy(rows_hbm, rows, local_sem)
    load.start()
    load.wait()
    odd, high = lax.rem(me, 2), me // 2
    got[pl.ds(16 * odd, 16), high] = rows[0:16, me]
    got_taps[me] = rows[16:18, me]
    wait_for(NZ - 1)

    def taps_to(k):
        peer = lax.rem(me + k, NZ)
        return pltpu.make_async_remote_copy(
            src_ref=rows.at[pl.ds(16, 2), peer], dst_ref=got_taps.at[me], send_sem=send_sem.at[0, k],
            recv_sem=recv_sem.at[0, k], device_id={"z": peer}, device_id_type=MESH)

    def values_to(k):
        peer = lax.rem(me + k, NZ)
        return pltpu.make_async_remote_copy(
            src_ref=rows.at[pl.ds(0, 16), peer], dst_ref=got.at[pl.ds(16 * odd, 16), high], send_sem=send_sem.at[1, k],
            recv_sem=recv_sem.at[1, k], device_id={"z": peer}, device_id_type=MESH)

    def back_to(k):
        peer = lax.rem(me + k, NZ)
        return pltpu.make_async_remote_copy(
            src_ref=results.at[pl.ds(16 * lax.rem(peer, 2), 16), peer // 2], dst_ref=back.at[:, me],
            send_sem=send_sem.at[2, k], recv_sem=recv_sem.at[2, k], device_id={"z": peer}, device_id_type=MESH)

    order = (8, 7, 9, 6, 10, 5, 11, 4, 12, 3, 13, 2, 14, 1, 15)
    for k in order:
        taps_to(k).start()
    for k in order:
        values_to(k).start()
    for k in order:
        taps_to(k).wait()
    each(0, NZ, lambda z: lags.__setitem__(pl.ds(pl.multiple_of(4 * z, 4), 4), got_taps[z].astype(F32).reshape(4, 128)))

    row = lax.broadcasted_iota(jnp.int32, (128, 128), 0)
    col = lax.broadcasted_iota(jnp.int32, (128, 128), 1)
    after = col >= row
    zero = jnp.zeros((128, 128), F32)

    def turned_rows(j, c):
        line = lags[pl.ds(2 * j + c, 1), :]
        return pltpu.roll(jnp.broadcast_to(line, (128, 128)), 0, 1, stride=1, stride_axis=0)

    for c in range(2):
        lanes = slice(c * 128, (c + 1) * 128)
        first = turned_rows(0, c)
        toeplitz[0, :, lanes] = jnp.where(after, first, zero).astype(BF16)

        def place(j, before):
            current = turned_rows(j, c)
            toeplitz[j, :, lanes] = jnp.where(after, current, before).astype(BF16)
            return current

        last = lax.fori_loop(1, 32, place, first)
        toeplitz[32, :, lanes] = jnp.where(after, zero, last).astype(BF16)

    for k in order:
        values_to(k).wait()

    def unpack(l):
        x = got[l].astype(F32).reshape(16, 128)
        blocks[32 + l] = x.astype(BF16)
        blocks[l] = jnp.concatenate([jnp.zeros((2, 128), F32), x[:14]], axis=0).astype(BF16)

    each(0, 32, unpack)

    def left(j):
        return blocks[pl.ds(32 - j, 32)].reshape(512, 128)

    total[...] = jnp.dot(left(32), toeplitz[32], preferred_element_type=F32)

    def add(k):
        pair = jnp.concatenate([left(2 * k), left(2 * k + 1)], axis=1)
        total[...] += jnp.dot(pair, toeplitz[pl.ds(2 * k, 2)].reshape(256, 256), preferred_element_type=F32)

    each(0, 16, add)

    even = lax.rem(lax.broadcasted_iota(jnp.int32, (16, 128), 0), 2) == 0

    def pick(l):
        both = total[pl.ds(pl.multiple_of(16 * l, 16), 16), :]
        results[l] = jnp.where(even, both[:, :128], both[:, 128:]).astype(BF16).reshape(8, 2, 128)

    each(0, 32, pick)
    for k in order:
        back_to(k).start()
    back[:, me] = results[pl.ds(16 * odd, 16), high]
    for k in order:
        back_to(k).wait()


def mix_kernel(
    back_hbm, values_hbm, gates_hbm, skip_ref, weight_hbm, out_ref,
    back, values, gates, weight, got, hidden, gathered, local_sem, send_sem, recv_sem, side_send, side_recv,
):
    me = lax.axis_index("w")
    my_ch = lax.axis_index("ch")
    greet("w", NW)
    greet("ch", 4)
    loads = [
        pltpu.make_async_copy(source, target, local_sem.at[k])
        for k, (source, target) in enumerate(
            ((back_hbm, back), (values_hbm, values), (gates_hbm, gates), (weight_hbm, weight))
        )
    ]
    for load in loads:
        load.start()
    loads[0].wait()
    got[:, me] = back[pl.ds(2 * me, 2)]
    wait_for(NW - 1 + 3)

    def part_to(k):
        peer = lax.rem(me + k, NW)
        return pltpu.make_async_remote_copy(
            src_ref=back.at[pl.ds(2 * peer, 2)], dst_ref=got.at[:, me], send_sem=send_sem.at[k],
            recv_sem=recv_sem.at[k], device_id={"w": peer}, device_id_type=MESH)

    order = (4, 3, 5, 2, 6, 1, 7)
    for k in order:
        part_to(k).start()
    loads[1].wait()
    loads[2].wait()
    for k in order:
        part_to(k).wait()

    for half in range(2):
        rows = slice(half * 128, (half + 1) * 128)
        convolved = got[half].astype(F32).reshape(256, 128).T
        hidden[rows, :] = (gates[rows, :] * (convolved + skip_ref[...] * values[rows, :])).astype(BF16)

    def side_to(k):
        return pltpu.make_async_remote_copy(
            src_ref=hidden, dst_ref=gathered.at[k - 1], send_sem=side_send.at[k - 1],
            recv_sem=side_recv.at[k - 1], device_id={"ch": lax.rem(my_ch + k, 4)}, device_id_type=MESH)

    for k in (2, 1, 3):
        side_to(k).start()
    loads[3].wait()

    def part(block, channel):
        rows = pl.ds(pl.multiple_of(channel * 256, 256), 256)
        return jnp.dot(block, weight[rows, :], preferred_element_type=F32)

    out_ref[...] = part(hidden[...], my_ch)
    for k in (1, 3, 2):
        side_to(k).wait()
        out_ref[...] += part(gathered[k - 1], lax.rem(my_ch + 4 - k, 4))


def body(values, gates, filter_taps, skip, out_weight):
    dma = pltpu.SemaphoreType.DMA
    vmem = pl.BlockSpec(memory_space=VMEM)
    spread = pl.pallas_call(
        spread_kernel,
        out_shape=jax.ShapeDtypeStruct((18, NZ, 2, 128), BF16),
        in_specs=[ANY, ANY],
        out_specs=vmem,
        scratch_shapes=[
            VMEM((256, 256), F32), VMEM((32, 256), F32), VMEM((2, NW, NZ, 2, 128), BF16),
            VMEM((NW, NZ, 2, 128), BF16), VMEM((NW, NZ, 2, 128), BF16), dma((2,)), dma((2, NW)), dma((2, NW)),
        ],
        compiler_params=pltpu.CompilerParams(collective_id=0, has_side_effects=True),
    )(values, filter_taps)
    back = pl.pallas_call(
        convolve_kernel,
        out_shape=jax.ShapeDtypeStruct((16, NZ, 2, 128), BF16),
        in_specs=[ANY],
        out_specs=vmem,
        scratch_shapes=[
            VMEM((18, NZ, 2, 128), BF16), VMEM((32, 8, 2, 128), BF16), VMEM((NZ, 2, 2, 128), BF16),
            VMEM((64, 16, 128), BF16), VMEM((64, 128), F32), VMEM((33, 128, 256), BF16), VMEM((512, 256), F32),
            VMEM((32, 8, 2, 128), BF16), dma, dma((3, NZ)), dma((3, NZ)),
        ],
        compiler_params=pltpu.CompilerParams(collective_id=1, has_side_effects=True),
    )(spread)
    return pl.pallas_call(
        mix_kernel,
        out_shape=jax.ShapeDtypeStruct((256, 512), F32),
        in_specs=[ANY, ANY, ANY, vmem, ANY],
        out_specs=vmem,
        scratch_shapes=[
            VMEM((16, NZ, 2, 128), BF16), VMEM((256, 256), F32), VMEM((256, 256), F32), VMEM((1024, 512), BF16),
            VMEM((2, NW, NZ, 2, 128), BF16), VMEM((256, 256), BF16), VMEM((3, 256, 256), BF16),
            dma((4,)), dma((NW,)), dma((NW,)), dma((3,)), dma((3,)),
        ],
        compiler_params=pltpu.CompilerParams(collective_id=2, has_side_effects=True),
    )(back, values, gates, skip.reshape(1, 256), out_weight)


def solution(mesh):
    torus = Mesh(mesh.devices.reshape(NZ, NW, 4), ("z", "w", "ch"))
    tokens = ("z", "w")
    return jax.shard_map(
        body,
        mesh=torus,
        in_specs=(P(tokens, "ch"), P(tokens, "ch"), P(tokens, "ch"), P("ch"), P(None, "ch")),
        out_specs=P(tokens, "ch"),
        check_vma=False,
    )
```

```python
import functools

import jax
import jax.numpy as jnp
from jax import lax
from jax.experimental import pallas as pl
from jax.experimental.pallas import tpu as pltpu
from jax.sharding import Mesh
from jax.sharding import PartitionSpec as P

MESH = pl.DeviceIdType.MESH
F32 = jnp.float32
BF16 = jnp.bfloat16
VMEM = pltpu.VMEM
ANY = pl.BlockSpec(memory_space=pl.ANY)
NZ, NW = 16, 8


def each(low, high, step):
    def run(k, _):
        step(k)
        return 0

    lax.fori_loop(low, high, run, 0)


def greet(axis, size):
    me = lax.axis_index(axis)
    barrier = pltpu.get_barrier_semaphore()
    for k in range(1, size):
        pl.semaphore_signal(barrier, inc=1, device_id={axis: lax.rem(me + k, size)}, device_id_type=MESH)


def wait_for(count):
    pl.semaphore_wait(pltpu.get_barrier_semaphore(), count)


def spread_kernel(values_hbm, taps_hbm, out, values, taps, send_values, send_taps, got_taps, local_sem, send_sem, recv_sem):
    me = lax.axis_index("w")
    greet("w", NW)
    loads = [
        pltpu.make_async_copy(taps_hbm, taps, local_sem.at[0]),
        pltpu.make_async_copy(values_hbm, values, local_sem.at[1]),
    ]
    for load in loads:
        load.start()
    loads[0].wait()
    own = jnp.concatenate([taps[...], jnp.zeros((96, 256), F32)], axis=0)
    own = pltpu.roll(own.T, 32 * lax.rem(me, 4), 1)
    send_taps[...] = own.astype(BF16).reshape(NW, NZ, 2, 128)
    loads[1].wait()
    for half in range(2):
        turned = values[half * 128:(half + 1) * 128, :].T
        send_values[half] = turned.astype(BF16).reshape(NW, NZ, 2, 128)
    wait_for(NW - 1)

    def taps_to(k):
        peer = lax.rem(me + k, NW)
        return pltpu.make_async_remote_copy(
            src_ref=send_taps.at[peer], dst_ref=got_taps.at[k], send_sem=send_sem.at[0, k],
            recv_sem=recv_sem.at[0, k], device_id={"w": peer}, device_id_type=MESH)

    def values_to(k):
        peer = lax.rem(me + k, NW)
        return pltpu.make_async_remote_copy(
            src_ref=send_values.at[:, peer], dst_ref=out.at[pl.ds(2 * me, 2)], send_sem=send_sem.at[1, k],
            recv_sem=recv_sem.at[1, k], device_id={"w": peer}, device_id_type=MESH)

    order = (4, 3, 5, 2, 6, 1, 7)
    for k in order:
        taps_to(k).start()
        values_to(k).start()
    out[pl.ds(2 * me, 2)] = send_values[:, me]
    got_taps[0] = send_taps[me]
    for k in order:
        taps_to(k).wait()
    for half in range(2):
        from_w = lambda w: got_taps[lax.rem(me + NW - w, NW)]
        w = 4 * half
        out[16 + half] = (from_w(w) + from_w(w + 1)) + (from_w(w + 2) + from_w(w + 3))
    for k in order:
        values_to(k).wait()


def convolve_kernel(rows, back, got, got_taps, blocks, lags, toeplitz, results, send_sem, recv_sem):
    me = lax.axis_index("z")
    greet("z", NZ)
    odd, high = lax.rem(me, 2), me // 2
    got[pl.ds(16 * odd, 16), high] = rows[0:16, me]
    got_taps[me] = rows[16:18, me]
    wait_for(NZ - 1)

    def taps_to(k):
        peer = lax.rem(me + k, NZ)
        return pltpu.make_async_remote_copy(
            src_ref=rows.at[pl.ds(16, 2), peer], dst_ref=got_taps.at[me], send_sem=send_sem.at[0, k],
            recv_sem=recv_sem.at[0, k], device_id={"z": peer}, device_id_type=MESH)

    def values_to(k):
        peer = lax.rem(me + k, NZ)
        return pltpu.make_async_remote_copy(
            src_ref=rows.at[pl.ds(0, 16), peer], dst_ref=got.at[pl.ds(16 * odd, 16), high], send_sem=send_sem.at[1, k],
            recv_sem=recv_sem.at[1, k], device_id={"z": peer}, device_id_type=MESH)

    def back_to(k):
        peer = lax.rem(me + k, NZ)
        return pltpu.make_async_remote_copy(
            src_ref=results.at[pl.ds(16 * lax.rem(peer, 2), 16), peer // 2], dst_ref=back.at[:, me],
            send_sem=send_sem.at[2, k], recv_sem=recv_sem.at[2, k], device_id={"z": peer}, device_id_type=MESH)

    order = (8, 7, 9, 6, 10, 5, 11, 4, 12, 3, 13, 2, 14, 1, 15)
    for k in order:
        taps_to(k).start()
    for k in order:
        values_to(k).start()
    for k in order:
        taps_to(k).wait()
    lags[0:2] = jnp.zeros((2, 128), F32)
    lags[66:68] = jnp.zeros((2, 128), F32)
    for z in range(NZ):
        lags[2 + 4 * z:6 + 4 * z] = got_taps[z].astype(F32).reshape(4, 128)

    row = lax.broadcasted_iota(jnp.int32, (128, 128), 0)
    col = lax.broadcasted_iota(jnp.int32, (128, 128), 1)
    straight = col < 128 - row

    def place(step):
        for part in range(3):
            j = 3 * step + part
            for c in range(2):
                block = jnp.broadcast_to(lags[pl.ds(2 * j + 2 + c, 1), :], (128, 128))
                before = jnp.broadcast_to(lags[pl.ds(2 * j + c, 1), :], (128, 128))
                tile = pltpu.roll(jnp.where(straight, block, before), 0, 1, stride=1, stride_axis=0)
                toeplitz[j, :, c * 128:(c + 1) * 128] = tile.astype(BF16)

    each(0, 11, place)

    for k in order:
        values_to(k).wait()

    def unpack(step):
        for part in range(8):
            l = 8 * step + part
            x = got[l].astype(F32).reshape(16, 128)
            blocks[32 + l] = x.astype(BF16)
            blocks[l] = jnp.concatenate([jnp.zeros((2, 128), F32), x[:14]], axis=0).astype(BF16)

    each(0, 4, unpack)

    even = lax.rem(lax.broadcasted_iota(jnp.int32, (256, 128), 0), 2) == 0

    for side in range(2):
        def left(j):
            return blocks[32 - j + 16 * side:48 - j + 16 * side].reshape(256, 128)

        sums = jnp.dot(left(32), toeplitz[32], preferred_element_type=F32)
        for k in range(16):
            pair = jnp.concatenate([left(2 * k), left(2 * k + 1)], axis=1)
            sums += jnp.dot(pair, toeplitz[2 * k:2 * k + 2].reshape(256, 256), preferred_element_type=F32)
        chosen = jnp.where(even, sums[:, :128], sums[:, 128:])
        results[16 * side:16 * side + 16] = chosen.astype(BF16).reshape(16, 8, 2, 128)
    for k in order:
        back_to(k).start()
    back[:, me] = results[pl.ds(16 * odd, 16), high]
    for k in order:
        back_to(k).wait()


def mix_kernel(
    back, values_hbm, gates_hbm, skip_ref, weight_hbm, out_ref,
    values, gates, weight, got, hidden, gathered, local_sem, send_sem, recv_sem, side_send, side_recv,
):
    me = lax.axis_index("w")
    my_ch = lax.axis_index("ch")
    greet("w", NW)
    greet("ch", 4)
    loads = [
        pltpu.make_async_copy(source, target, local_sem.at[k])
        for k, (source, target) in enumerate(
            ((values_hbm, values), (gates_hbm, gates), (weight_hbm, weight))
        )
    ]
    for load in loads:
        load.start()
    got[:, me] = back[pl.ds(2 * me, 2)]
    wait_for(NW - 1 + 3)

    def part_to(k):
        peer = lax.rem(me + k, NW)
        return pltpu.make_async_remote_copy(
            src_ref=back.at[pl.ds(2 * peer, 2)], dst_ref=got.at[:, me], send_sem=send_sem.at[k],
            recv_sem=recv_sem.at[k], device_id={"w": peer}, device_id_type=MESH)

    order = (4, 3, 5, 2, 6, 1, 7)
    for k in order:
        part_to(k).start()
    loads[0].wait()
    loads[1].wait()
    for k in order:
        part_to(k).wait()

    for half in range(2):
        rows = slice(half * 128, (half + 1) * 128)
        convolved = got[half].astype(F32).reshape(256, 128).T
        hidden[rows, :] = (gates[rows, :] * (convolved + skip_ref[...] * values[rows, :])).astype(BF16)

    def side_to(k):
        return pltpu.make_async_remote_copy(
            src_ref=hidden, dst_ref=gathered.at[k - 1], send_sem=side_send.at[k - 1],
            recv_sem=side_recv.at[k - 1], device_id={"ch": lax.rem(my_ch + k, 4)}, device_id_type=MESH)

    for k in (2, 1, 3):
        side_to(k).start()
    loads[2].wait()

    def part(block, channel):
        rows = pl.ds(pl.multiple_of(channel * 256, 256), 256)
        return jnp.dot(block, weight[rows, :], preferred_element_type=F32)

    out_ref[...] = part(hidden[...], my_ch)
    for k in (1, 3, 2):
        side_to(k).wait()
        out_ref[...] += part(gathered[k - 1], lax.rem(my_ch + 4 - k, 4))


def body(values, gates, filter_taps, skip, out_weight):
    dma = pltpu.SemaphoreType.DMA
    vmem = pl.BlockSpec(memory_space=VMEM)
    spread = pl.pallas_call(
        spread_kernel,
        out_shape=pltpu.VMEM((18, NZ, 2, 128), BF16),
        in_specs=[ANY, ANY],
        out_specs=vmem,
        scratch_shapes=[
            VMEM((256, 256), F32), VMEM((32, 256), F32), VMEM((2, NW, NZ, 2, 128), BF16),
            VMEM((NW, NZ, 2, 128), BF16), VMEM((NW, NZ, 2, 128), BF16), dma((2,)), dma((2, NW)), dma((2, NW)),
        ],
        compiler_params=pltpu.CompilerParams(collective_id=0, has_side_effects=True),
    )(values, filter_taps)
    back = pl.pallas_call(
        convolve_kernel,
        out_shape=pltpu.VMEM((16, NZ, 2, 128), BF16),
        in_specs=[vmem],
        out_specs=vmem,
        scratch_shapes=[
            VMEM((32, 8, 2, 128), BF16), VMEM((NZ, 2, 2, 128), BF16),
            VMEM((64, 16, 128), BF16), VMEM((68, 128), F32), VMEM((33, 128, 256), BF16),
            VMEM((32, 8, 2, 128), BF16), dma((3, NZ)), dma((3, NZ)),
        ],
        compiler_params=pltpu.CompilerParams(collective_id=1, has_side_effects=True),
    )(pltpu.with_memory_space_constraint(spread, VMEM))
    return pl.pallas_call(
        mix_kernel,
        out_shape=jax.ShapeDtypeStruct((256, 512), F32),
        in_specs=[vmem, ANY, ANY, vmem, ANY],
        out_specs=vmem,
        scratch_shapes=[
            VMEM((256, 256), F32), VMEM((256, 256), F32), VMEM((1024, 512), BF16),
            VMEM((2, NW, NZ, 2, 128), BF16), VMEM((256, 256), BF16), VMEM((3, 256, 256), BF16),
            dma((3,)), dma((NW,)), dma((NW,)), dma((3,)), dma((3,)),
        ],
        compiler_params=pltpu.CompilerParams(collective_id=2, has_side_effects=True),
    )(pltpu.with_memory_space_constraint(back, VMEM), values, gates, skip.reshape(1, 256), out_weight)


def solution(mesh):
    torus = Mesh(mesh.devices.reshape(NZ, NW, 4), ("z", "w", "ch"))
    tokens = ("z", "w")
    return jax.shard_map(
        body,
        mesh=torus,
        in_specs=(P(tokens, "ch"), P(tokens, "ch"), P(tokens, "ch"), P("ch"), P(None, "ch")),
        out_specs=P(tokens, "ch"),
        check_vma=False,
    )
```

```python
import functools

import jax
import jax.numpy as jnp
from jax import lax
from jax.experimental import pallas as pl
from jax.experimental.pallas import tpu as pltpu
from jax.sharding import Mesh
from jax.sharding import PartitionSpec as P

MESH = pl.DeviceIdType.MESH
F32 = jnp.float32
BF16 = jnp.bfloat16
VMEM = pltpu.VMEM
ANY = pl.BlockSpec(memory_space=pl.ANY)
NZ, NW = 16, 8


def each(low, high, step):
    def run(k, _):
        step(k)
        return 0

    lax.fori_loop(low, high, run, 0)


def greet(axis, size):
    me = lax.axis_index(axis)
    barrier = pltpu.get_barrier_semaphore()
    for k in range(1, size):
        pl.semaphore_signal(barrier, inc=1, device_id={axis: lax.rem(me + k, size)}, device_id_type=MESH)


def wait_for(count):
    pl.semaphore_wait(pltpu.get_barrier_semaphore(), count)


def spread_kernel(values_hbm, taps_hbm, out, values, taps, send_values, send_taps, got_taps, local_sem, send_sem, recv_sem):
    me = lax.axis_index("w")
    greet("w", NW)
    loads = [
        pltpu.make_async_copy(taps_hbm, taps, local_sem.at[0]),
        pltpu.make_async_copy(values_hbm, values, local_sem.at[1]),
    ]
    for load in loads:
        load.start()
    loads[0].wait()
    own = jnp.concatenate([taps[...], jnp.zeros((96, 256), F32)], axis=0)
    own = pltpu.roll(own.T, 32 * lax.rem(me, 4), 1)
    send_taps[...] = own.astype(BF16).reshape(NW, NZ, 2, 128)
    loads[1].wait()
    for half in range(2):
        turned = values[half * 128:(half + 1) * 128, :].T
        send_values[half] = turned.astype(BF16).reshape(NW, NZ, 2, 128)
    wait_for(NW - 1)

    def taps_to(k):
        peer = lax.rem(me + k, NW)
        return pltpu.make_async_remote_copy(
            src_ref=send_taps.at[peer], dst_ref=got_taps.at[k], send_sem=send_sem.at[0, k],
            recv_sem=recv_sem.at[0, k], device_id={"w": peer}, device_id_type=MESH)

    def values_to(k):
        peer = lax.rem(me + k, NW)
        return pltpu.make_async_remote_copy(
            src_ref=send_values.at[:, peer], dst_ref=out.at[pl.ds(2 * me, 2)], send_sem=send_sem.at[1, k],
            recv_sem=recv_sem.at[1, k], device_id={"w": peer}, device_id_type=MESH)

    order = (4, 3, 5, 2, 6, 1, 7)
    for k in order:
        taps_to(k).start()
        values_to(k).start()
    out[pl.ds(2 * me, 2)] = send_values[:, me]
    got_taps[0] = send_taps[me]
    for k in order:
        taps_to(k).wait()
    for half in range(2):
        from_w = lambda w: got_taps[lax.rem(me + NW - w, NW)]
        w = 4 * half
        out[16 + half] = (from_w(w) + from_w(w + 1)) + (from_w(w + 2) + from_w(w + 3))
    for k in order:
        values_to(k).wait()


def convolve_kernel(rows, back, got, got_taps, blocks, lags, toeplitz, results, send_sem, recv_sem):
    me = lax.axis_index("z")
    greet("z", NZ)
    odd, high = lax.rem(me, 2), me // 2
    got[pl.ds(16 * odd, 16), high] = rows[0:16, me]
    got_taps[me] = rows[16:18, me]
    wait_for(NZ - 1)

    def taps_to(k):
        peer = lax.rem(me + k, NZ)
        return pltpu.make_async_remote_copy(
            src_ref=rows.at[pl.ds(16, 2), peer], dst_ref=got_taps.at[me], send_sem=send_sem.at[0, k],
            recv_sem=recv_sem.at[0, k], device_id={"z": peer}, device_id_type=MESH)

    def values_to(k):
        peer = lax.rem(me + k, NZ)
        return pltpu.make_async_remote_copy(
            src_ref=rows.at[pl.ds(0, 16), peer], dst_ref=got.at[pl.ds(16 * odd, 16), high], send_sem=send_sem.at[1, k],
            recv_sem=recv_sem.at[1, k], device_id={"z": peer}, device_id_type=MESH)

    def back_to(k):
        peer = lax.rem(me + k, NZ)
        return pltpu.make_async_remote_copy(
            src_ref=results.at[pl.ds(16 * lax.rem(peer, 2), 16), peer // 2], dst_ref=back.at[:, me],
            send_sem=send_sem.at[2, k], recv_sem=recv_sem.at[2, k], device_id={"z": peer}, device_id_type=MESH)

    order = (8, 7, 9, 6, 10, 5, 11, 4, 12, 3, 13, 2, 14, 1, 15)
    for k in order:
        taps_to(k).start()
    for k in order:
        values_to(k).start()
    for k in order:
        taps_to(k).wait()
    lags[0:2] = jnp.zeros((2, 128), F32)
    lags[66:68] = jnp.zeros((2, 128), F32)
    for z in range(NZ):
        lags[2 + 4 * z:6 + 4 * z] = got_taps[z].astype(F32).reshape(4, 128)

    row = lax.broadcasted_iota(jnp.int32, (128, 128), 0)
    col = lax.broadcasted_iota(jnp.int32, (128, 128), 1)
    straight = col < 128 - row

    def place(step):
        for part in range(3):
            j = 3 * step + part
            for c in range(2):
                block = jnp.broadcast_to(lags[pl.ds(2 * j + 2 + c, 1), :], (128, 128))
                before = jnp.broadcast_to(lags[pl.ds(2 * j + c, 1), :], (128, 128))
                tile = pltpu.roll(jnp.where(straight, block, before), 0, 1, stride=1, stride_axis=0)
                toeplitz[j, :, c * 128:(c + 1) * 128] = tile.astype(BF16)

    each(0, 11, place)

    for k in order:
        values_to(k).wait()

    def unpack(step):
        for part in range(8):
            l = 8 * step + part
            x = got[l].astype(F32).reshape(16, 128)
            blocks[32 + l] = x.astype(BF16)
            blocks[l] = jnp.concatenate([jnp.zeros((2, 128), F32), x[:14]], axis=0).astype(BF16)

    each(0, 4, unpack)

    even = lax.rem(lax.broadcasted_iota(jnp.int32, (256, 128), 0), 2) == 0

    for side in range(2):
        def left(j):
            return blocks[32 - j + 16 * side:48 - j + 16 * side].reshape(256, 128)

        sums = jnp.dot(left(32), toeplitz[32], preferred_element_type=F32)
        for k in range(16):
            pair = jnp.concatenate([left(2 * k), left(2 * k + 1)], axis=1)
            sums += jnp.dot(pair, toeplitz[2 * k:2 * k + 2].reshape(256, 256), preferred_element_type=F32)
        chosen = jnp.where(even, sums[:, :128], sums[:, 128:])
        results[16 * side:16 * side + 16] = chosen.astype(BF16).reshape(16, 8, 2, 128)
    for k in order:
        back_to(k).start()
    back[:, me] = results[pl.ds(16 * odd, 16), high]
    for k in order:
        back_to(k).wait()


def mix_kernel(
    back, values_hbm, gates_hbm, skip_ref, weight_hbm, gathered, weight,
    values, gates, got, local_sem, send_sem, recv_sem, right_send, left_recv, left_send, right_recv, on_send, on_recv,
):
    me = lax.axis_index("w")
    my_ch = lax.axis_index("ch")
    right, left, across = lax.rem(my_ch + 1, 4), lax.rem(my_ch + 3, 4), lax.rem(my_ch + 2, 4)
    greet("w", NW)
    barrier = pltpu.get_barrier_semaphore()
    for peer in (left, right):
        pl.semaphore_signal(barrier, inc=1, device_id={"ch": peer}, device_id_type=MESH)
    loads = [
        pltpu.make_async_copy(source, target, local_sem.at[k])
        for k, (source, target) in enumerate(((values_hbm, values), (gates_hbm, gates), (weight_hbm, weight)))
    ]
    for load in loads:
        load.start()
    got[:, me] = back[pl.ds(2 * me, 2)]
    wait_for(NW - 1 + 2)

    def part_to(k):
        peer = lax.rem(me + k, NW)
        return pltpu.make_async_remote_copy(
            src_ref=back.at[pl.ds(2 * peer, 2)], dst_ref=got.at[:, me], send_sem=send_sem.at[k],
            recv_sem=recv_sem.at[k], device_id={"w": peer}, device_id_type=MESH)

    order = (4, 3, 5, 2, 6, 1, 7)
    for k in order:
        part_to(k).start()
    loads[0].wait()
    loads[1].wait()
    for k in order:
        part_to(k).wait()

    def piece(slot, quarter):
        return gathered.at[slot, pl.ds(64 * quarter, 64)]

    def to_right(quarter):
        return pltpu.make_async_remote_copy(
            src_ref=piece(my_ch, quarter), dst_ref=piece(my_ch, quarter), send_sem=right_send.at[quarter],
            recv_sem=left_recv.at[quarter], device_id={"ch": right}, device_id_type=MESH)

    def to_left(quarter):
        return pltpu.make_async_remote_copy(
            src_ref=piece(my_ch, quarter), dst_ref=piece(my_ch, quarter), send_sem=left_send.at[quarter],
            recv_sem=right_recv.at[quarter], device_id={"ch": left}, device_id_type=MESH)

    def pass_on(quarter):
        source, target = (left, right) if quarter < 2 else (right, left)
        return pltpu.make_async_remote_copy(
            src_ref=piece(source, quarter), dst_ref=piece(source, quarter), send_sem=on_send.at[quarter],
            recv_sem=on_recv.at[quarter], device_id={"ch": target}, device_id_type=MESH)

    for half in range(2):
        rows = slice(half * 128, (half + 1) * 128)
        convolved = got[half].astype(F32).reshape(256, 128).T
        hidden = (gates[rows, :] * (convolved + skip_ref[...] * values[rows, :])).astype(BF16)
        gathered[my_ch, rows, :] = hidden
        for quarter in (2 * half, 2 * half + 1):
            (to_left if half else to_right)(quarter).start()
    for quarter in (2, 3):
        to_right(quarter).start()
    for quarter in (0, 1):
        to_left(quarter).start()
    for first, second in ((0, 2), (1, 3)):
        to_right(first).wait_recv()
        pass_on(first).start()
        to_left(second).wait_recv()
        pass_on(second).start()
    loads[2].wait()
    for quarter in (2, 3):
        to_right(quarter).wait_recv()
    for quarter in (0, 1):
        to_left(quarter).wait_recv()
    for quarter in range(4):
        to_right(quarter).wait_send()
        to_left(quarter).wait_send()
        pass_on(quarter).wait()


def output_kernel(gathered, weight, out_hbm, out, out_sem):
    def store(half):
        rows = pl.ds(128 * half, 128)
        return pltpu.make_async_copy(out.at[rows], out_hbm.at[rows], out_sem.at[half])

    for half in range(2):
        rows = slice(128 * half, 128 * half + 128)
        for side in range(2):
            lanes = slice(256 * side, 256 * side + 256)
            sums = jnp.dot(gathered[0, rows, :], weight[0:256, lanes], preferred_element_type=F32)
            for k in range(1, 4):
                sums += jnp.dot(gathered[k, rows, :], weight[256 * k:256 * k + 256, lanes], preferred_element_type=F32)
            out[rows, lanes] = sums
        store(half).start()
    for half in range(2):
        store(half).wait()


def body(values, gates, filter_taps, skip, out_weight):
    dma = pltpu.SemaphoreType.DMA
    vmem = pl.BlockSpec(memory_space=VMEM)
    spread = pl.pallas_call(
        spread_kernel,
        out_shape=pltpu.VMEM((18, NZ, 2, 128), BF16),
        in_specs=[ANY, ANY],
        out_specs=vmem,
        scratch_shapes=[
            VMEM((256, 256), F32), VMEM((32, 256), F32), VMEM((2, NW, NZ, 2, 128), BF16),
            VMEM((NW, NZ, 2, 128), BF16), VMEM((NW, NZ, 2, 128), BF16), dma((2,)), dma((2, NW)), dma((2, NW)),
        ],
        compiler_params=pltpu.CompilerParams(collective_id=0, has_side_effects=True),
    )(values, filter_taps)
    back = pl.pallas_call(
        convolve_kernel,
        out_shape=pltpu.VMEM((16, NZ, 2, 128), BF16),
        in_specs=[vmem],
        out_specs=vmem,
        scratch_shapes=[
            VMEM((32, 8, 2, 128), BF16), VMEM((NZ, 2, 2, 128), BF16),
            VMEM((64, 16, 128), BF16), VMEM((68, 128), F32), VMEM((33, 128, 256), BF16),
            VMEM((32, 8, 2, 128), BF16), dma((3, NZ)), dma((3, NZ)),
        ],
        compiler_params=pltpu.CompilerParams(collective_id=1, has_side_effects=True),
    )(pltpu.with_memory_space_constraint(spread, VMEM))
    near = lambda x: pltpu.with_memory_space_constraint(x, VMEM)
    gathered, weight = pl.pallas_call(
        mix_kernel,
        out_shape=(VMEM((4, 256, 256), BF16), VMEM((1024, 512), BF16)),
        in_specs=[vmem, ANY, ANY, vmem, ANY],
        out_specs=(vmem, vmem),
        scratch_shapes=[
            VMEM((256, 256), F32), VMEM((256, 256), F32), VMEM((2, NW, NZ, 2, 128), BF16),
            dma((3,)), dma((NW,)), dma((NW,)), dma((4,)), dma((4,)), dma((4,)), dma((4,)), dma((4,)), dma((4,)),
        ],
        compiler_params=pltpu.CompilerParams(collective_id=2, has_side_effects=True),
    )(near(back), values, gates, skip.reshape(1, 256), out_weight)
    return pl.pallas_call(
        output_kernel,
        out_shape=jax.ShapeDtypeStruct((256, 512), F32),
        in_specs=[vmem, vmem],
        out_specs=ANY,
        scratch_shapes=[VMEM((256, 512), F32), dma((2,))],
    )(near(gathered), near(weight))


def solution(mesh):
    torus = Mesh(mesh.devices.reshape(NZ, NW, 4), ("z", "w", "ch"))
    tokens = ("z", "w")
    return jax.shard_map(
        body,
        mesh=torus,
        in_specs=(P(tokens, "ch"), P(tokens, "ch"), P(tokens, "ch"), P("ch"), P(None, "ch")),
        out_specs=P(tokens, "ch"),
        check_vma=False,
    )
```

```python
import functools

import jax
import jax.numpy as jnp
from jax import lax
from jax.experimental import pallas as pl
from jax.experimental.pallas import tpu as pltpu
from jax.sharding import Mesh
from jax.sharding import PartitionSpec as P

MESH = pl.DeviceIdType.MESH
F32 = jnp.float32
BF16 = jnp.bfloat16
VMEM = pltpu.VMEM
ANY = pl.BlockSpec(memory_space=pl.ANY)
NZ, NW = 16, 8


def each(low, high, step):
    def run(k, _):
        step(k)
        return 0

    lax.fori_loop(low, high, run, 0)


def greet(axis, size):
    me = lax.axis_index(axis)
    barrier = pltpu.get_barrier_semaphore()
    for k in range(1, size):
        pl.semaphore_signal(barrier, inc=1, device_id={axis: lax.rem(me + k, size)}, device_id_type=MESH)


def wait_for(count):
    pl.semaphore_wait(pltpu.get_barrier_semaphore(), count)


def spread_kernel(values_hbm, taps_hbm, out, values, taps, send_values, send_taps, got_taps, local_sem, send_sem, recv_sem):
    me = lax.axis_index("w")
    greet("w", NW)
    loads = [
        pltpu.make_async_copy(taps_hbm, taps, local_sem.at[0]),
        pltpu.make_async_copy(values_hbm, values, local_sem.at[1]),
    ]
    for load in loads:
        load.start()
    loads[0].wait()
    own = jnp.concatenate([taps[...], jnp.zeros((96, 256), F32)], axis=0)
    turned = own.T
    packed = turned[0:64] + pltpu.roll(turned[64:128], 32, 1)
    packed += pltpu.roll(turned[128:192], 64, 1) + pltpu.roll(turned[192:256], 96, 1)
    send_taps[...] = packed.astype(BF16).reshape(NW, 8, 128)
    loads[1].wait()
    for half in range(2):
        turned = values[half * 128:(half + 1) * 128, :].T
        for w in range(NW):
            own = jnp.concatenate([turned[64 * q + 8 * w:64 * q + 8 * w + 8] for q in range(4)], axis=0)
            send_values[half, w] = own.astype(BF16).reshape(NZ, 2, 128)
    wait_for(NW - 1)

    def taps_to(k):
        peer = lax.rem(me + k, NW)
        return pltpu.make_async_remote_copy(
            src_ref=send_taps.at[peer], dst_ref=got_taps.at[k], send_sem=send_sem.at[0, k],
            recv_sem=recv_sem.at[0, k], device_id={"w": peer}, device_id_type=MESH)

    def values_to(k):
        peer = lax.rem(me + k, NW)
        return pltpu.make_async_remote_copy(
            src_ref=send_values.at[:, peer], dst_ref=out.at[pl.ds(2 * me, 2)], send_sem=send_sem.at[1, k],
            recv_sem=recv_sem.at[1, k], device_id={"w": peer}, device_id_type=MESH)

    order = (4, 3, 5, 2, 6, 1, 7)
    for k in order:
        taps_to(k).start()
        values_to(k).start()
    out[pl.ds(2 * me, 2)] = send_values[:, me]
    got_taps[0] = send_taps[me]
    for k in order:
        taps_to(k).wait()
    lane = lax.broadcasted_iota(jnp.int32, (8, 128), 1)
    for half in range(2):
        parts = [got_taps[lax.rem(me + NW - w, NW)].astype(F32) for w in range(4 * half, 4 * half + 4)]
        rows = []
        for q in range(4):
            line = pltpu.roll(parts[3], 32 * ((3 - q) % 4), 1) if q != 3 else parts[3]
            for k in range(3):
                moved = pltpu.roll(parts[k], 32 * ((k - q) % 4), 1) if k != q else parts[k]
                line = jnp.where((lane >= 32 * k) & (lane < 32 * k + 32), moved, line)
            rows.append(line)
        out[16 + half] = jnp.concatenate(rows, axis=0).astype(BF16).reshape(NZ, 2, 128)
    for k in order:
        values_to(k).wait()


def convolve_kernel(rows, back, got, got_taps, blocks, lags, toeplitz, results, send_sem, recv_sem):
    me = lax.axis_index("z")
    greet("z", NZ)
    odd, high = lax.rem(me, 2), me // 2
    got[pl.ds(16 * odd, 16), high] = rows[0:16, me]
    got_taps[me] = rows[16:18, me]
    wait_for(NZ - 1)

    def taps_to(k):
        peer = lax.rem(me + k, NZ)
        return pltpu.make_async_remote_copy(
            src_ref=rows.at[pl.ds(16, 2), peer], dst_ref=got_taps.at[me], send_sem=send_sem.at[0, k],
            recv_sem=recv_sem.at[0, k], device_id={"z": peer}, device_id_type=MESH)

    def values_to(k):
        peer = lax.rem(me + k, NZ)
        return pltpu.make_async_remote_copy(
            src_ref=rows.at[pl.ds(0, 16), peer], dst_ref=got.at[pl.ds(16 * odd, 16), high], send_sem=send_sem.at[1, k],
            recv_sem=recv_sem.at[1, k], device_id={"z": peer}, device_id_type=MESH)

    def back_to(k):
        peer = lax.rem(me + k, NZ)
        return pltpu.make_async_remote_copy(
            src_ref=results.at[pl.ds(16 * lax.rem(peer, 2), 16), peer // 2], dst_ref=back.at[:, me],
            send_sem=send_sem.at[2, k], recv_sem=recv_sem.at[2, k], device_id={"z": peer}, device_id_type=MESH)

    order = (8, 7, 9, 6, 10, 5, 11, 4, 12, 3, 13, 2, 14, 1, 15)
    for k in order:
        taps_to(k).start()
    for k in order:
        values_to(k).start()
    for k in order:
        taps_to(k).wait()
    lags[0:2] = jnp.zeros((2, 128), F32)
    lags[66:68] = jnp.zeros((2, 128), F32)
    for z in range(NZ):
        lags[2 + 4 * z:6 + 4 * z] = got_taps[z].astype(F32).reshape(4, 128)

    row = lax.broadcasted_iota(jnp.int32, (128, 128), 0)
    col = lax.broadcasted_iota(jnp.int32, (128, 128), 1)
    straight = col < 128 - row

    def place(step):
        for part in range(3):
            j = 3 * step + part
            for c in range(2):
                block = jnp.broadcast_to(lags[pl.ds(2 * j + 2 + c, 1), :], (128, 128))
                before = jnp.broadcast_to(lags[pl.ds(2 * j + c, 1), :], (128, 128))
                tile = pltpu.roll(jnp.where(straight, block, before), 0, 1, stride=1, stride_axis=0)
                toeplitz[j, :, c * 128:(c + 1) * 128] = tile.astype(BF16)

    each(0, 11, place)

    for k in order:
        values_to(k).wait()

    def unpack(step):
        for part in range(8):
            l = 8 * step + part
            x = got[l].astype(F32).reshape(16, 128)
            blocks[32 + l] = x.astype(BF16)
            blocks[l] = jnp.concatenate([jnp.zeros((2, 128), F32), x[:14]], axis=0).astype(BF16)

    each(0, 4, unpack)

    even = lax.rem(lax.broadcasted_iota(jnp.int32, (256, 128), 0), 2) == 0

    for side in range(2):
        def left(j):
            return blocks[32 - j + 16 * side:48 - j + 16 * side].reshape(256, 128)

        sums = jnp.dot(left(32), toeplitz[32], preferred_element_type=F32)
        for k in range(16):
            pair = jnp.concatenate([left(2 * k), left(2 * k + 1)], axis=1)
            sums += jnp.dot(pair, toeplitz[2 * k:2 * k + 2].reshape(256, 256), preferred_element_type=F32)
        chosen = jnp.where(even, sums[:, :128], sums[:, 128:])
        results[16 * side:16 * side + 16] = chosen.astype(BF16).reshape(16, 8, 2, 128)
    for k in order:
        back_to(k).start()
    back[:, me] = results[pl.ds(16 * odd, 16), high]
    for k in order:
        back_to(k).wait()


def mix_kernel(
    back, values_hbm, gates_hbm, skip_ref, weight_hbm, gathered, weight,
    values, gates, got, local_sem, send_sem, recv_sem, right_send, left_recv, left_send, right_recv, on_send, on_recv,
):
    me = lax.axis_index("w")
    my_ch = lax.axis_index("ch")
    right, left, across = lax.rem(my_ch + 1, 4), lax.rem(my_ch + 3, 4), lax.rem(my_ch + 2, 4)
    greet("w", NW)
    barrier = pltpu.get_barrier_semaphore()
    for peer in (left, right):
        pl.semaphore_signal(barrier, inc=1, device_id={"ch": peer}, device_id_type=MESH)
    loads = [
        pltpu.make_async_copy(source, target, local_sem.at[k])
        for k, (source, target) in enumerate(((values_hbm, values), (gates_hbm, gates), (weight_hbm, weight)))
    ]
    for load in loads:
        load.start()
    got[:, me] = back[pl.ds(2 * me, 2)]
    wait_for(NW - 1 + 2)

    def part_to(k):
        peer = lax.rem(me + k, NW)
        return pltpu.make_async_remote_copy(
            src_ref=back.at[pl.ds(2 * peer, 2)], dst_ref=got.at[:, me], send_sem=send_sem.at[k],
            recv_sem=recv_sem.at[k], device_id={"w": peer}, device_id_type=MESH)

    order = (4, 3, 5, 2, 6, 1, 7)
    for k in order:
        part_to(k).start()
    loads[0].wait()
    loads[1].wait()
    for k in order:
        part_to(k).wait()

    def piece(slot, quarter):
        return gathered.at[slot, pl.ds(64 * quarter, 64)]

    def to_right(quarter):
        return pltpu.make_async_remote_copy(
            src_ref=piece(my_ch, quarter), dst_ref=piece(my_ch, quarter), send_sem=right_send.at[quarter],
            recv_sem=left_recv.at[quarter], device_id={"ch": right}, device_id_type=MESH)

    def to_left(quarter):
        return pltpu.make_async_remote_copy(
            src_ref=piece(my_ch, quarter), dst_ref=piece(my_ch, quarter), send_sem=left_send.at[quarter],
            recv_sem=right_recv.at[quarter], device_id={"ch": left}, device_id_type=MESH)

    def pass_on(quarter):
        source, target = (left, right) if quarter < 2 else (right, left)
        return pltpu.make_async_remote_copy(
            src_ref=piece(source, quarter), dst_ref=piece(source, quarter), send_sem=on_send.at[quarter],
            recv_sem=on_recv.at[quarter], device_id={"ch": target}, device_id_type=MESH)

    for half in range(2):
        rows = slice(half * 128, (half + 1) * 128)
        arrived = got[half].astype(F32).reshape(256, 128)
        convolved = jnp.concatenate(
            [arrived[32 * w + 8 * q:32 * w + 8 * q + 8] for q in range(4) for w in range(NW)], axis=0).T
        hidden = (gates[rows, :] * (convolved + skip_ref[...] * values[rows, :])).astype(BF16)
        gathered[my_ch, rows, :] = hidden
        for quarter in (2 * half, 2 * half + 1):
            (to_left if half else to_right)(quarter).start()
    for quarter in (2, 3):
        to_right(quarter).start()
    for quarter in (0, 1):
        to_left(quarter).start()
    for first, second in ((0, 2), (1, 3)):
        to_right(first).wait_recv()
        pass_on(first).start()
        to_left(second).wait_recv()
        pass_on(second).start()
    loads[2].wait()
    for quarter in (2, 3):
        to_right(quarter).wait_recv()
    for quarter in (0, 1):
        to_left(quarter).wait_recv()
    for quarter in range(4):
        to_right(quarter).wait_send()
        to_left(quarter).wait_send()
        pass_on(quarter).wait()


def output_kernel(gathered, weight, out_hbm, out, out_sem):
    def store(half):
        rows = pl.ds(128 * half, 128)
        return pltpu.make_async_copy(out.at[rows], out_hbm.at[rows], out_sem.at[half])

    for half in range(2):
        rows = slice(128 * half, 128 * half + 128)
        for side in range(2):
            lanes = slice(256 * side, 256 * side + 256)
            sums = jnp.dot(gathered[0, rows, :], weight[0:256, lanes], preferred_element_type=F32)
            for k in range(1, 4):
                sums += jnp.dot(gathered[k, rows, :], weight[256 * k:256 * k + 256, lanes], preferred_element_type=F32)
            out[rows, lanes] = sums
        store(half).start()
    for half in range(2):
        store(half).wait()


def body(values, gates, filter_taps, skip, out_weight):
    dma = pltpu.SemaphoreType.DMA
    vmem = pl.BlockSpec(memory_space=VMEM)
    spread = pl.pallas_call(
        spread_kernel,
        out_shape=pltpu.VMEM((18, NZ, 2, 128), BF16),
        in_specs=[ANY, ANY],
        out_specs=vmem,
        scratch_shapes=[
            VMEM((256, 256), F32), VMEM((32, 256), F32), VMEM((2, NW, NZ, 2, 128), BF16),
            VMEM((NW, 8, 128), BF16), VMEM((NW, 8, 128), BF16), dma((2,)), dma((2, NW)), dma((2, NW)),
        ],
        compiler_params=pltpu.CompilerParams(collective_id=0, has_side_effects=True),
    )(values, filter_taps)
    back = pl.pallas_call(
        convolve_kernel,
        out_shape=pltpu.VMEM((16, NZ, 2, 128), BF16),
        in_specs=[vmem],
        out_specs=vmem,
        scratch_shapes=[
            VMEM((32, 8, 2, 128), BF16), VMEM((NZ, 2, 2, 128), BF16),
            VMEM((64, 16, 128), BF16), VMEM((68, 128), F32), VMEM((33, 128, 256), BF16),
            VMEM((32, 8, 2, 128), BF16), dma((3, NZ)), dma((3, NZ)),
        ],
        compiler_params=pltpu.CompilerParams(collective_id=1, has_side_effects=True),
    )(pltpu.with_memory_space_constraint(spread, VMEM))
    near = lambda x: pltpu.with_memory_space_constraint(x, VMEM)
    gathered, weight = pl.pallas_call(
        mix_kernel,
        out_shape=(VMEM((4, 256, 256), BF16), VMEM((1024, 512), BF16)),
        in_specs=[vmem, ANY, ANY, vmem, ANY],
        out_specs=(vmem, vmem),
        scratch_shapes=[
            VMEM((256, 256), F32), VMEM((256, 256), F32), VMEM((2, NW, NZ, 2, 128), BF16),
            dma((3,)), dma((NW,)), dma((NW,)), dma((4,)), dma((4,)), dma((4,)), dma((4,)), dma((4,)), dma((4,)),
        ],
        compiler_params=pltpu.CompilerParams(collective_id=2, has_side_effects=True),
    )(near(back), values, gates, skip.reshape(1, 256), out_weight)
    return pl.pallas_call(
        output_kernel,
        out_shape=jax.ShapeDtypeStruct((256, 512), F32),
        in_specs=[vmem, vmem],
        out_specs=ANY,
        scratch_shapes=[VMEM((256, 512), F32), dma((2,))],
    )(near(gathered), near(weight))


def solution(mesh):
    torus = Mesh(mesh.devices.reshape(NZ, NW, 4), ("z", "w", "ch"))
    tokens = ("z", "w")
    return jax.shard_map(
        body,
        mesh=torus,
        in_specs=(P(tokens, "ch"), P(tokens, "ch"), P(tokens, "ch"), P("ch"), P(None, "ch")),
        out_specs=P(tokens, "ch"),
        check_vma=False,
    )
```

```python
import functools

import jax
import jax.numpy as jnp
from jax import lax
from jax.experimental import pallas as pl
from jax.experimental.pallas import tpu as pltpu
from jax.sharding import Mesh
from jax.sharding import PartitionSpec as P

MESH = pl.DeviceIdType.MESH
F32 = jnp.float32
BF16 = jnp.bfloat16
VMEM = pltpu.VMEM
ANY = pl.BlockSpec(memory_space=pl.ANY)
NZ, NW = 16, 8


def each(low, high, step):
    def run(k, _):
        step(k)
        return 0

    lax.fori_loop(low, high, run, 0)


def greet(axis, size):
    me = lax.axis_index(axis)
    barrier = pltpu.get_barrier_semaphore()
    for k in range(1, size):
        pl.semaphore_signal(barrier, inc=1, device_id={axis: lax.rem(me + k, size)}, device_id_type=MESH)


def wait_for(count):
    pl.semaphore_wait(pltpu.get_barrier_semaphore(), count)


def convolve_kernel(
    values_hbm, taps_hbm, back, values, taps, send_values, send_taps, near_taps, rows, got, got_taps, blocks, lags,
    toeplitz, results, local_sem, near_send, near_recv, send_sem, recv_sem,
):
    at = lax.axis_index("w")
    me = lax.axis_index("z")
    greet("z", NZ)
    greet("w", NW)
    loads = [
        pltpu.make_async_copy(taps_hbm, taps, local_sem.at[0]),
        pltpu.make_async_copy(values_hbm, values, local_sem.at[1]),
    ]
    for load in loads:
        load.start()
    loads[0].wait()
    own = jnp.concatenate([taps[...], jnp.zeros((96, 256), F32)], axis=0)
    turned = own.T
    packed = turned[0:64] + pltpu.roll(turned[64:128], 32, 1)
    packed += pltpu.roll(turned[128:192], 64, 1) + pltpu.roll(turned[192:256], 96, 1)
    send_taps[...] = packed.astype(BF16).reshape(NW, 8, 128)
    loads[1].wait()
    for half in range(2):
        turned = values[half * 128:(half + 1) * 128, :].T
        for w in range(NW):
            own = jnp.concatenate([turned[64 * q + 8 * w:64 * q + 8 * w + 8] for q in range(4)], axis=0)
            send_values[half, w] = own.astype(BF16).reshape(NZ, 2, 128)
    wait_for(NW - 1 + NZ - 1)

    def taps_near(k):
        peer = lax.rem(at + k, NW)
        return pltpu.make_async_remote_copy(
            src_ref=send_taps.at[peer], dst_ref=near_taps.at[k], send_sem=near_send.at[0, k],
            recv_sem=near_recv.at[0, k], device_id={"w": peer}, device_id_type=MESH)

    def values_near(k):
        peer = lax.rem(at + k, NW)
        return pltpu.make_async_remote_copy(
            src_ref=send_values.at[:, peer], dst_ref=rows.at[pl.ds(2 * at, 2)], send_sem=near_send.at[1, k],
            recv_sem=near_recv.at[1, k], device_id={"w": peer}, device_id_type=MESH)

    near_order = (4, 3, 5, 2, 6, 1, 7)
    for k in near_order:
        taps_near(k).start()
        values_near(k).start()
    rows[pl.ds(2 * at, 2)] = send_values[:, at]
    near_taps[0] = send_taps[at]
    for k in near_order:
        taps_near(k).wait()
    lane = lax.broadcasted_iota(jnp.int32, (8, 128), 1)
    for half in range(2):
        parts = [near_taps[lax.rem(at + NW - w, NW)].astype(F32) for w in range(4 * half, 4 * half + 4)]
        lines = []
        for q in range(4):
            line = pltpu.roll(parts[3], 32 * ((3 - q) % 4), 1) if q != 3 else parts[3]
            for k in range(3):
                moved = pltpu.roll(parts[k], 32 * ((k - q) % 4), 1) if k != q else parts[k]
                line = jnp.where((lane >= 32 * k) & (lane < 32 * k + 32), moved, line)
            lines.append(line)
        rows[16 + half] = jnp.concatenate(lines, axis=0).astype(BF16).reshape(NZ, 2, 128)
    for k in near_order:
        values_near(k).wait()

    odd, high = lax.rem(me, 2), me // 2
    got[pl.ds(16 * odd, 16), high] = rows[0:16, me]
    got_taps[me] = rows[16:18, me]

    def taps_to(k):
        peer = lax.rem(me + k, NZ)
        return pltpu.make_async_remote_copy(
            src_ref=rows.at[pl.ds(16, 2), peer], dst_ref=got_taps.at[me], send_sem=send_sem.at[0, k],
            recv_sem=recv_sem.at[0, k], device_id={"z": peer}, device_id_type=MESH)

    def values_to(k):
        peer = lax.rem(me + k, NZ)
        return pltpu.make_async_remote_copy(
            src_ref=rows.at[pl.ds(0, 16), peer], dst_ref=got.at[pl.ds(16 * odd, 16), high], send_sem=send_sem.at[1, k],
            recv_sem=recv_sem.at[1, k], device_id={"z": peer}, device_id_type=MESH)

    def back_to(k):
        peer = lax.rem(me + k, NZ)
        return pltpu.make_async_remote_copy(
            src_ref=results.at[pl.ds(16 * lax.rem(peer, 2), 16), peer // 2], dst_ref=back.at[:, me],
            send_sem=send_sem.at[2, k], recv_sem=recv_sem.at[2, k], device_id={"z": peer}, device_id_type=MESH)

    order = (8, 7, 9, 6, 10, 5, 11, 4, 12, 3, 13, 2, 14, 1, 15)
    for k in order:
        taps_to(k).start()
    for k in order:
        values_to(k).start()
    for k in order:
        taps_to(k).wait()
    lags[0:2] = jnp.zeros((2, 128), F32)
    lags[66:68] = jnp.zeros((2, 128), F32)
    for z in range(NZ):
        lags[2 + 4 * z:6 + 4 * z] = got_taps[z].astype(F32).reshape(4, 128)

    row = lax.broadcasted_iota(jnp.int32, (128, 128), 0)
    col = lax.broadcasted_iota(jnp.int32, (128, 128), 1)
    straight = col < 128 - row

    def place(step):
        for part in range(3):
            j = 3 * step + part
            for c in range(2):
                block = jnp.broadcast_to(lags[pl.ds(2 * j + 2 + c, 1), :], (128, 128))
                before = jnp.broadcast_to(lags[pl.ds(2 * j + c, 1), :], (128, 128))
                tile = pltpu.roll(jnp.where(straight, block, before), 0, 1, stride=1, stride_axis=0)
                toeplitz[j, :, c * 128:(c + 1) * 128] = tile.astype(BF16)

    each(0, 11, place)

    for k in order:
        values_to(k).wait()

    def unpack(step):
        for part in range(8):
            l = 8 * step + part
            x = got[l].astype(F32).reshape(16, 128)
            blocks[32 + l] = x.astype(BF16)
            blocks[l] = jnp.concatenate([jnp.zeros((2, 128), F32), x[:14]], axis=0).astype(BF16)

    each(0, 4, unpack)

    even = lax.rem(lax.broadcasted_iota(jnp.int32, (256, 128), 0), 2) == 0

    for side in range(2):
        def left(j):
            return blocks[32 - j + 16 * side:48 - j + 16 * side].reshape(256, 128)

        sums = jnp.dot(left(32), toeplitz[32], preferred_element_type=F32)
        for k in range(16):
            pair = jnp.concatenate([left(2 * k), left(2 * k + 1)], axis=1)
            sums += jnp.dot(pair, toeplitz[2 * k:2 * k + 2].reshape(256, 256), preferred_element_type=F32)
        chosen = jnp.where(even, sums[:, :128], sums[:, 128:])
        results[16 * side:16 * side + 16] = chosen.astype(BF16).reshape(16, 8, 2, 128)
    for k in order:
        back_to(k).start()
    back[:, me] = results[pl.ds(16 * odd, 16), high]
    for k in order:
        back_to(k).wait()


def mix_kernel(
    back, values_hbm, gates_hbm, skip_ref, weight_hbm, gathered, weight,
    values, gates, got, local_sem, send_sem, recv_sem, right_send, left_recv, left_send, right_recv, on_send, on_recv,
):
    me = lax.axis_index("w")
    my_ch = lax.axis_index("ch")
    right, left, across = lax.rem(my_ch + 1, 4), lax.rem(my_ch + 3, 4), lax.rem(my_ch + 2, 4)
    greet("w", NW)
    barrier = pltpu.get_barrier_semaphore()
    for peer in (left, right):
        pl.semaphore_signal(barrier, inc=1, device_id={"ch": peer}, device_id_type=MESH)
    loads = [
        pltpu.make_async_copy(source, target, local_sem.at[k])
        for k, (source, target) in enumerate(((values_hbm, values), (gates_hbm, gates), (weight_hbm, weight)))
    ]
    for load in loads:
        load.start()
    got[:, me] = back[pl.ds(2 * me, 2)]
    wait_for(NW - 1 + 2)

    def part_to(k):
        peer = lax.rem(me + k, NW)
        return pltpu.make_async_remote_copy(
            src_ref=back.at[pl.ds(2 * peer, 2)], dst_ref=got.at[:, me], send_sem=send_sem.at[k],
            recv_sem=recv_sem.at[k], device_id={"w": peer}, device_id_type=MESH)

    order = (4, 3, 5, 2, 6, 1, 7)
    for k in order:
        part_to(k).start()
    loads[0].wait()
    loads[1].wait()
    for k in order:
        part_to(k).wait()

    def piece(slot, quarter):
        return gathered.at[slot, pl.ds(64 * quarter, 64)]

    def to_right(quarter):
        return pltpu.make_async_remote_copy(
            src_ref=piece(my_ch, quarter), dst_ref=piece(my_ch, quarter), send_sem=right_send.at[quarter],
            recv_sem=left_recv.at[quarter], device_id={"ch": right}, device_id_type=MESH)

    def to_left(quarter):
        return pltpu.make_async_remote_copy(
            src_ref=piece(my_ch, quarter), dst_ref=piece(my_ch, quarter), send_sem=left_send.at[quarter],
            recv_sem=right_recv.at[quarter], device_id={"ch": left}, device_id_type=MESH)

    def pass_on(quarter):
        source, target = (left, right) if quarter < 2 else (right, left)
        return pltpu.make_async_remote_copy(
            src_ref=piece(source, quarter), dst_ref=piece(source, quarter), send_sem=on_send.at[quarter],
            recv_sem=on_recv.at[quarter], device_id={"ch": target}, device_id_type=MESH)

    for half in range(2):
        rows = slice(half * 128, (half + 1) * 128)
        arrived = got[half].astype(F32).reshape(256, 128)
        convolved = jnp.concatenate(
            [arrived[32 * w + 8 * q:32 * w + 8 * q + 8] for q in range(4) for w in range(NW)], axis=0).T
        hidden = (gates[rows, :] * (convolved + skip_ref[...] * values[rows, :])).astype(BF16)
        gathered[my_ch, rows, :] = hidden
        for quarter in (2 * half, 2 * half + 1):
            (to_left if half else to_right)(quarter).start()
    for quarter in (2, 3):
        to_right(quarter).start()
    for quarter in (0, 1):
        to_left(quarter).start()
    for first, second in ((0, 2), (1, 3)):
        to_right(first).wait_recv()
        pass_on(first).start()
        to_left(second).wait_recv()
        pass_on(second).start()
    loads[2].wait()
    for quarter in (2, 3):
        to_right(quarter).wait_recv()
    for quarter in (0, 1):
        to_left(quarter).wait_recv()
    for quarter in range(4):
        to_right(quarter).wait_send()
        to_left(quarter).wait_send()
        pass_on(quarter).wait()


def output_kernel(gathered, weight, out_hbm, out, out_sem):
    def store(half):
        rows = pl.ds(128 * half, 128)
        return pltpu.make_async_copy(out.at[rows], out_hbm.at[rows], out_sem.at[half])

    for half in range(2):
        rows = slice(128 * half, 128 * half + 128)
        for side in range(2):
            lanes = slice(256 * side, 256 * side + 256)
            sums = jnp.dot(gathered[0, rows, :], weight[0:256, lanes], preferred_element_type=F32)
            for k in range(1, 4):
                sums += jnp.dot(gathered[k, rows, :], weight[256 * k:256 * k + 256, lanes], preferred_element_type=F32)
            out[rows, lanes] = sums
        store(half).start()
    for half in range(2):
        store(half).wait()


def body(values, gates, filter_taps, skip, out_weight):
    dma = pltpu.SemaphoreType.DMA
    vmem = pl.BlockSpec(memory_space=VMEM)
    back = pl.pallas_call(
        convolve_kernel,
        out_shape=VMEM((16, NZ, 2, 128), BF16),
        in_specs=[ANY, ANY],
        out_specs=vmem,
        scratch_shapes=[
            VMEM((256, 256), F32), VMEM((32, 256), F32), VMEM((2, NW, NZ, 2, 128), BF16),
            VMEM((NW, 8, 128), BF16), VMEM((NW, 8, 128), BF16), VMEM((18, NZ, 2, 128), BF16),
            VMEM((32, 8, 2, 128), BF16), VMEM((NZ, 2, 2, 128), BF16), VMEM((64, 16, 128), BF16),
            VMEM((68, 128), F32), VMEM((33, 128, 256), BF16), VMEM((32, 8, 2, 128), BF16),
            dma((2,)), dma((2, NW)), dma((2, NW)), dma((3, NZ)), dma((3, NZ)),
        ],
        compiler_params=pltpu.CompilerParams(collective_id=1, has_side_effects=True),
    )(values, filter_taps)
    near = lambda x: pltpu.with_memory_space_constraint(x, VMEM)
    gathered, weight = pl.pallas_call(
        mix_kernel,
        out_shape=(VMEM((4, 256, 256), BF16), VMEM((1024, 512), BF16)),
        in_specs=[vmem, ANY, ANY, vmem, ANY],
        out_specs=(vmem, vmem),
        scratch_shapes=[
            VMEM((256, 256), F32), VMEM((256, 256), F32), VMEM((2, NW, NZ, 2, 128), BF16),
            dma((3,)), dma((NW,)), dma((NW,)), dma((4,)), dma((4,)), dma((4,)), dma((4,)), dma((4,)), dma((4,)),
        ],
        compiler_params=pltpu.CompilerParams(collective_id=2, has_side_effects=True),
    )(near(back), values, gates, skip.reshape(1, 256), out_weight)
    return pl.pallas_call(
        output_kernel,
        out_shape=jax.ShapeDtypeStruct((256, 512), F32),
        in_specs=[vmem, vmem],
        out_specs=ANY,
        scratch_shapes=[VMEM((256, 512), F32), dma((2,))],
    )(near(gathered), near(weight))


def solution(mesh):
    torus = Mesh(mesh.devices.reshape(NZ, NW, 4), ("z", "w", "ch"))
    tokens = ("z", "w")
    return jax.shard_map(
        body,
        mesh=torus,
        in_specs=(P(tokens, "ch"), P(tokens, "ch"), P(tokens, "ch"), P("ch"), P(None, "ch")),
        out_specs=P(tokens, "ch"),
        check_vma=False,
    )
```

```python
import functools

import jax
import jax.numpy as jnp
from jax import lax
from jax.experimental import pallas as pl
from jax.experimental.pallas import tpu as pltpu
from jax.sharding import Mesh
from jax.sharding import PartitionSpec as P

MESH = pl.DeviceIdType.MESH
F32 = jnp.float32
BF16 = jnp.bfloat16
VMEM = pltpu.VMEM
ANY = pl.BlockSpec(memory_space=pl.ANY)
NZ, NW = 16, 8


def each(low, high, step):
    def run(k, _):
        step(k)
        return 0

    lax.fori_loop(low, high, run, 0)


def greet(axis, size):
    me = lax.axis_index(axis)
    barrier = pltpu.get_barrier_semaphore()
    for k in range(1, size):
        pl.semaphore_signal(barrier, inc=1, device_id={axis: lax.rem(me + k, size)}, device_id_type=MESH)


def wait_for(count):
    pl.semaphore_wait(pltpu.get_barrier_semaphore(), count)


def convolve_kernel(
    values_hbm, taps_hbm, back, values, taps, send_values, send_taps, near_taps, rows, got, got_taps, blocks, lags,
    toeplitz, results, local_sem, near_send, near_recv, send_sem, recv_sem, back_send, back_recv,
):
    at = lax.axis_index("w")
    me = lax.axis_index("z")
    greet("z", NZ)
    greet("w", NW)
    loads = [
        pltpu.make_async_copy(taps_hbm, taps, local_sem.at[0]),
        pltpu.make_async_copy(values_hbm, values, local_sem.at[1]),
    ]
    for load in loads:
        load.start()
    loads[0].wait()
    own = jnp.concatenate([taps[...], jnp.zeros((96, 256), F32)], axis=0)
    turned = own.T
    packed = turned[0:64] + pltpu.roll(turned[64:128], 32, 1)
    packed += pltpu.roll(turned[128:192], 64, 1) + pltpu.roll(turned[192:256], 96, 1)
    send_taps[...] = packed.astype(BF16).reshape(NW, 8, 128)
    loads[1].wait()
    for half in range(2):
        turned = values[half * 128:(half + 1) * 128, :].T
        for w in range(NW):
            own = jnp.concatenate([turned[64 * q + 8 * w:64 * q + 8 * w + 8] for q in range(4)], axis=0)
            send_values[half, w] = own.astype(BF16).reshape(NZ, 2, 128)
    wait_for(NW - 1 + NZ - 1)

    def taps_near(k):
        peer = lax.rem(at + k, NW)
        return pltpu.make_async_remote_copy(
            src_ref=send_taps.at[peer], dst_ref=near_taps.at[k], send_sem=near_send.at[0, k],
            recv_sem=near_recv.at[0, k], device_id={"w": peer}, device_id_type=MESH)

    def values_near(k):
        peer = lax.rem(at + k, NW)
        return pltpu.make_async_remote_copy(
            src_ref=send_values.at[:, peer], dst_ref=rows.at[pl.ds(2 * at, 2)], send_sem=near_send.at[1, k],
            recv_sem=near_recv.at[1, k], device_id={"w": peer}, device_id_type=MESH)

    near_order = (4, 3, 5, 2, 6, 1, 7)
    for k in near_order:
        taps_near(k).start()
        values_near(k).start()
    rows[pl.ds(2 * at, 2)] = send_values[:, at]
    near_taps[0] = send_taps[at]
    for k in near_order:
        taps_near(k).wait()
    lane = lax.broadcasted_iota(jnp.int32, (8, 128), 1)
    for half in range(2):
        parts = [near_taps[lax.rem(at + NW - w, NW)].astype(F32) for w in range(4 * half, 4 * half + 4)]
        lines = []
        for q in range(4):
            line = pltpu.roll(parts[3], 32 * ((3 - q) % 4), 1) if q != 3 else parts[3]
            for k in range(3):
                moved = pltpu.roll(parts[k], 32 * ((k - q) % 4), 1) if k != q else parts[k]
                line = jnp.where((lane >= 32 * k) & (lane < 32 * k + 32), moved, line)
            lines.append(line)
        rows[16 + half] = jnp.concatenate(lines, axis=0).astype(BF16).reshape(NZ, 2, 128)
    for k in near_order:
        values_near(k).wait()

    odd, high = lax.rem(me, 2), me // 2
    got[pl.ds(16 * odd, 16), high] = rows[0:16, me]
    got_taps[me] = rows[16:18, me]

    def taps_to(k):
        peer = lax.rem(me + k, NZ)
        return pltpu.make_async_remote_copy(
            src_ref=rows.at[pl.ds(16, 2), peer], dst_ref=got_taps.at[me], send_sem=send_sem.at[0, k],
            recv_sem=recv_sem.at[0, k], device_id={"z": peer}, device_id_type=MESH)

    def values_to(k):
        peer = lax.rem(me + k, NZ)
        return pltpu.make_async_remote_copy(
            src_ref=rows.at[pl.ds(0, 16), peer], dst_ref=got.at[pl.ds(16 * odd, 16), high], send_sem=send_sem.at[1, k],
            recv_sem=recv_sem.at[1, k], device_id={"z": peer}, device_id_type=MESH)

    def back_to(k):
        peer = lax.rem(NW * me + at + k, NW * NZ)
        z, w = peer // NW, lax.rem(peer, NW)
        return pltpu.make_async_remote_copy(
            src_ref=results.at[pl.ds(16 * lax.rem(z, 2) + 2 * w, 2), z // 2], dst_ref=back.at[:, at, me],
            send_sem=back_send.at[k], recv_sem=back_recv.at[k], device_id={"z": z, "w": w}, device_id_type=MESH)

    order = (8, 7, 9, 6, 10, 5, 11, 4, 12, 3, 13, 2, 14, 1, 15)
    for k in order:
        taps_to(k).start()
    for k in order:
        values_to(k).start()
    for k in order:
        taps_to(k).wait()
    lags[0:2] = jnp.zeros((2, 128), F32)
    lags[66:68] = jnp.zeros((2, 128), F32)
    for z in range(NZ):
        lags[2 + 4 * z:6 + 4 * z] = got_taps[z].astype(F32).reshape(4, 128)

    row = lax.broadcasted_iota(jnp.int32, (128, 128), 0)
    col = lax.broadcasted_iota(jnp.int32, (128, 128), 1)
    straight = col < 128 - row

    def place(step):
        for part in range(3):
            j = 3 * step + part
            for c in range(2):
                block = jnp.broadcast_to(lags[pl.ds(2 * j + 2 + c, 1), :], (128, 128))
                before = jnp.broadcast_to(lags[pl.ds(2 * j + c, 1), :], (128, 128))
                tile = pltpu.roll(jnp.where(straight, block, before), 0, 1, stride=1, stride_axis=0)
                toeplitz[j, :, c * 128:(c + 1) * 128] = tile.astype(BF16)

    each(0, 11, place)

    for k in order:
        values_to(k).wait()

    def unpack(step):
        for part in range(8):
            l = 8 * step + part
            x = got[l].astype(F32).reshape(16, 128)
            blocks[32 + l] = x.astype(BF16)
            blocks[l] = jnp.concatenate([jnp.zeros((2, 128), F32), x[:14]], axis=0).astype(BF16)

    each(0, 4, unpack)

    even = lax.rem(lax.broadcasted_iota(jnp.int32, (256, 128), 0), 2) == 0

    for side in range(2):
        def left(j):
            return blocks[32 - j + 16 * side:48 - j + 16 * side].reshape(256, 128)

        sums = jnp.dot(left(32), toeplitz[32], preferred_element_type=F32)
        for k in range(16):
            pair = jnp.concatenate([left(2 * k), left(2 * k + 1)], axis=1)
            sums += jnp.dot(pair, toeplitz[2 * k:2 * k + 2].reshape(256, 256), preferred_element_type=F32)
        chosen = jnp.where(even, sums[:, :128], sums[:, 128:])
        results[16 * side:16 * side + 16] = chosen.astype(BF16).reshape(16, 8, 2, 128)
    back_to(64).start()

    def far_first(k):
        back_to(64 + k).start()
        back_to(64 - k).start()

    each(1, 64, far_first)
    back[:, at, me] = results[pl.ds(16 * odd + 2 * at, 2), high]
    each(1, 128, lambda k: back_to(k).wait())


def mix_kernel(
    back, values_hbm, gates_hbm, skip_ref, weight_hbm, gathered, weight,
    values, gates, local_sem, right_send, left_recv, left_send, right_recv, on_send, on_recv,
):
    my_ch = lax.axis_index("ch")
    right, left, across = lax.rem(my_ch + 1, 4), lax.rem(my_ch + 3, 4), lax.rem(my_ch + 2, 4)
    barrier = pltpu.get_barrier_semaphore()
    for peer in (left, right):
        pl.semaphore_signal(barrier, inc=1, device_id={"ch": peer}, device_id_type=MESH)
    loads = [
        pltpu.make_async_copy(source, target, local_sem.at[k])
        for k, (source, target) in enumerate(((values_hbm, values), (gates_hbm, gates), (weight_hbm, weight)))
    ]
    for load in loads:
        load.start()
    loads[0].wait()
    loads[1].wait()
    wait_for(2)

    def piece(slot, quarter):
        return gathered.at[slot, pl.ds(64 * quarter, 64)]

    def to_right(quarter):
        return pltpu.make_async_remote_copy(
            src_ref=piece(my_ch, quarter), dst_ref=piece(my_ch, quarter), send_sem=right_send.at[quarter],
            recv_sem=left_recv.at[quarter], device_id={"ch": right}, device_id_type=MESH)

    def to_left(quarter):
        return pltpu.make_async_remote_copy(
            src_ref=piece(my_ch, quarter), dst_ref=piece(my_ch, quarter), send_sem=left_send.at[quarter],
            recv_sem=right_recv.at[quarter], device_id={"ch": left}, device_id_type=MESH)

    def pass_on(quarter):
        source, target = (left, right) if quarter < 2 else (right, left)
        return pltpu.make_async_remote_copy(
            src_ref=piece(source, quarter), dst_ref=piece(source, quarter), send_sem=on_send.at[quarter],
            recv_sem=on_recv.at[quarter], device_id={"ch": target}, device_id_type=MESH)

    for half in range(2):
        rows = slice(half * 128, (half + 1) * 128)
        arrived = back[half].astype(F32).reshape(256, 128)
        convolved = jnp.concatenate(
            [arrived[32 * w + 8 * q:32 * w + 8 * q + 8] for q in range(4) for w in range(NW)], axis=0).T
        hidden = (gates[rows, :] * (convolved + skip_ref[...] * values[rows, :])).astype(BF16)
        gathered[my_ch, rows, :] = hidden
        for quarter in (2 * half, 2 * half + 1):
            (to_left if half else to_right)(quarter).start()
    for quarter in (2, 3):
        to_right(quarter).start()
    for quarter in (0, 1):
        to_left(quarter).start()
    for first, second in ((0, 2), (1, 3)):
        to_right(first).wait_recv()
        pass_on(first).start()
        to_left(second).wait_recv()
        pass_on(second).start()
    loads[2].wait()
    for quarter in (2, 3):
        to_right(quarter).wait_recv()
    for quarter in (0, 1):
        to_left(quarter).wait_recv()
    for quarter in range(4):
        to_right(quarter).wait_send()
        to_left(quarter).wait_send()
        pass_on(quarter).wait()


def output_kernel(gathered, weight, out_hbm, out, out_sem):
    def store(half):
        rows = pl.ds(128 * half, 128)
        return pltpu.make_async_copy(out.at[rows], out_hbm.at[rows], out_sem.at[half])

    for half in range(2):
        rows = slice(128 * half, 128 * half + 128)
        for side in range(2):
            lanes = slice(256 * side, 256 * side + 256)
            sums = jnp.dot(gathered[0, rows, :], weight[0:256, lanes], preferred_element_type=F32)
            for k in range(1, 4):
                sums += jnp.dot(gathered[k, rows, :], weight[256 * k:256 * k + 256, lanes], preferred_element_type=F32)
            out[rows, lanes] = sums
        store(half).start()
    for half in range(2):
        store(half).wait()


def body(values, gates, filter_taps, skip, out_weight):
    dma = pltpu.SemaphoreType.DMA
    vmem = pl.BlockSpec(memory_space=VMEM)
    back = pl.pallas_call(
        convolve_kernel,
        out_shape=VMEM((2, NW, NZ, 2, 128), BF16),
        in_specs=[ANY, ANY],
        out_specs=vmem,
        scratch_shapes=[
            VMEM((256, 256), F32), VMEM((32, 256), F32), VMEM((2, NW, NZ, 2, 128), BF16),
            VMEM((NW, 8, 128), BF16), VMEM((NW, 8, 128), BF16), VMEM((18, NZ, 2, 128), BF16),
            VMEM((32, 8, 2, 128), BF16), VMEM((NZ, 2, 2, 128), BF16), VMEM((64, 16, 128), BF16),
            VMEM((68, 128), F32), VMEM((33, 128, 256), BF16), VMEM((32, 8, 2, 128), BF16),
            dma((2,)), dma((2, NW)), dma((2, NW)), dma((2, NZ)), dma((2, NZ)), dma((128,)), dma((128,)),
        ],
        compiler_params=pltpu.CompilerParams(collective_id=1, has_side_effects=True),
    )(values, filter_taps)
    near = lambda x: pltpu.with_memory_space_constraint(x, VMEM)
    gathered, weight = pl.pallas_call(
        mix_kernel,
        out_shape=(VMEM((4, 256, 256), BF16), VMEM((1024, 512), BF16)),
        in_specs=[vmem, ANY, ANY, vmem, ANY],
        out_specs=(vmem, vmem),
        scratch_shapes=[
            VMEM((256, 256), F32), VMEM((256, 256), F32),
            dma((3,)), dma((4,)), dma((4,)), dma((4,)), dma((4,)), dma((4,)), dma((4,)),
        ],
        compiler_params=pltpu.CompilerParams(collective_id=2, has_side_effects=True),
    )(near(back), values, gates, skip.reshape(1, 256), out_weight)
    return pl.pallas_call(
        output_kernel,
        out_shape=jax.ShapeDtypeStruct((256, 512), F32),
        in_specs=[vmem, vmem],
        out_specs=ANY,
        scratch_shapes=[VMEM((256, 512), F32), dma((2,))],
    )(near(gathered), near(weight))


def solution(mesh):
    torus = Mesh(mesh.devices.reshape(NZ, NW, 4), ("z", "w", "ch"))
    tokens = ("z", "w")
    return jax.shard_map(
        body,
        mesh=torus,
        in_specs=(P(tokens, "ch"), P(tokens, "ch"), P(tokens, "ch"), P("ch"), P(None, "ch")),
        out_specs=P(tokens, "ch"),
        check_vma=False,
    )
```

```python
import functools

import jax
import jax.numpy as jnp
from jax import lax
from jax.experimental import pallas as pl
from jax.experimental.pallas import tpu as pltpu
from jax.sharding import Mesh
from jax.sharding import PartitionSpec as P

MESH = pl.DeviceIdType.MESH
F32 = jnp.float32
BF16 = jnp.bfloat16
VMEM = pltpu.VMEM
ANY = pl.BlockSpec(memory_space=pl.ANY)
NZ, NW = 16, 8


def each(low, high, step):
    def run(k, _):
        step(k)
        return 0

    lax.fori_loop(low, high, run, 0)


def greet(axis, size):
    me = lax.axis_index(axis)
    barrier = pltpu.get_barrier_semaphore()
    for k in range(1, size):
        pl.semaphore_signal(barrier, inc=1, device_id={axis: lax.rem(me + k, size)}, device_id_type=MESH)


def wait_for(count):
    pl.semaphore_wait(pltpu.get_barrier_semaphore(), count)


def convolve_kernel(
    values_hbm, taps_hbm, back, values, taps, send_values, send_taps, near_taps, rows, got, got_taps, blocks, lags,
    toeplitz, results, local_sem, near_send, near_recv, send_sem, recv_sem, back_send, back_recv,
):
    at = lax.axis_index("w")
    me = lax.axis_index("z")
    greet("z", NZ)
    greet("w", NW)
    loads = [
        pltpu.make_async_copy(taps_hbm, taps, local_sem.at[0]),
        pltpu.make_async_copy(values_hbm, values, local_sem.at[1]),
    ]
    for load in loads:
        load.start()
    loads[0].wait()
    own = jnp.concatenate([taps[...], jnp.zeros((96, 256), F32)], axis=0)
    turned = own.T
    packed = turned[0:64] + pltpu.roll(turned[64:128], 32, 1)
    packed += pltpu.roll(turned[128:192], 64, 1) + pltpu.roll(turned[192:256], 96, 1)
    send_taps[...] = packed.astype(BF16).reshape(NW, 8, 128)
    loads[1].wait()
    for half in range(2):
        turned = values[half * 128:(half + 1) * 128, :].T
        for w in range(NW):
            own = jnp.concatenate([turned[64 * q + 8 * w:64 * q + 8 * w + 8] for q in range(4)], axis=0)
            send_values[half, w] = own.astype(BF16).reshape(NZ, 2, 128)
    wait_for(NW - 1 + NZ - 1)

    def taps_near(k):
        peer = lax.rem(at + k, NW)
        return pltpu.make_async_remote_copy(
            src_ref=send_taps.at[peer], dst_ref=near_taps.at[k], send_sem=near_send.at[0, k],
            recv_sem=near_recv.at[0, k], device_id={"w": peer}, device_id_type=MESH)

    def values_near(k):
        peer = lax.rem(at + k, NW)
        return pltpu.make_async_remote_copy(
            src_ref=send_values.at[:, peer], dst_ref=rows.at[pl.ds(2 * at, 2)], send_sem=near_send.at[1, k],
            recv_sem=near_recv.at[1, k], device_id={"w": peer}, device_id_type=MESH)

    near_order = (4, 3, 5, 2, 6, 1, 7)
    for k in near_order:
        taps_near(k).start()
        values_near(k).start()
    rows[pl.ds(2 * at, 2)] = send_values[:, at]
    near_taps[0] = send_taps[at]
    for k in near_order:
        taps_near(k).wait()
    lane = lax.broadcasted_iota(jnp.int32, (8, 128), 1)
    for half in range(2):
        parts = [near_taps[lax.rem(at + NW - w, NW)].astype(F32) for w in range(4 * half, 4 * half + 4)]
        lines = []
        for q in range(4):
            line = pltpu.roll(parts[3], 32 * ((3 - q) % 4), 1) if q != 3 else parts[3]
            for k in range(3):
                moved = pltpu.roll(parts[k], 32 * ((k - q) % 4), 1) if k != q else parts[k]
                line = jnp.where((lane >= 32 * k) & (lane < 32 * k + 32), moved, line)
            lines.append(line)
        rows[16 + half] = jnp.concatenate(lines, axis=0).astype(BF16).reshape(NZ, 2, 128)

    odd, high = lax.rem(me, 2), me // 2
    got_taps[me] = rows[16:18, me]

    def taps_to(k):
        peer = lax.rem(me + k, NZ)
        return pltpu.make_async_remote_copy(
            src_ref=rows.at[pl.ds(16, 2), peer], dst_ref=got_taps.at[me], send_sem=send_sem.at[0, k],
            recv_sem=recv_sem.at[0, k], device_id={"z": peer}, device_id_type=MESH)

    def values_to(k):
        peer = lax.rem(me + k, NZ)
        return pltpu.make_async_remote_copy(
            src_ref=rows.at[pl.ds(0, 16), peer], dst_ref=got.at[pl.ds(16 * odd, 16), high], send_sem=send_sem.at[1, k],
            recv_sem=recv_sem.at[1, k], device_id={"z": peer}, device_id_type=MESH)

    def back_to(k):
        peer = lax.rem(NW * me + at + k, NW * NZ)
        z, w = peer // NW, lax.rem(peer, NW)
        return pltpu.make_async_remote_copy(
            src_ref=results.at[pl.ds(16 * lax.rem(z, 2) + 2 * w, 2), z // 2], dst_ref=back.at[:, at, me],
            send_sem=back_send.at[k], recv_sem=back_recv.at[k], device_id={"z": z, "w": w}, device_id_type=MESH)

    order = (8, 7, 9, 6, 10, 5, 11, 4, 12, 3, 13, 2, 14, 1, 15)
    for k in order:
        taps_to(k).start()
    for k in near_order:
        values_near(k).wait()
    got[pl.ds(16 * odd, 16), high] = rows[0:16, me]
    for k in order:
        values_to(k).start()
    for k in order:
        taps_to(k).wait()
    lags[0:2] = jnp.zeros((2, 128), F32)
    lags[66:68] = jnp.zeros((2, 128), F32)
    for z in range(NZ):
        lags[2 + 4 * z:6 + 4 * z] = got_taps[z].astype(F32).reshape(4, 128)

    row = lax.broadcasted_iota(jnp.int32, (128, 128), 0)
    col = lax.broadcasted_iota(jnp.int32, (128, 128), 1)
    straight = col < 128 - row

    def place(step):
        for part in range(3):
            j = 3 * step + part
            for c in range(2):
                block = jnp.broadcast_to(lags[pl.ds(2 * j + 2 + c, 1), :], (128, 128))
                before = jnp.broadcast_to(lags[pl.ds(2 * j + c, 1), :], (128, 128))
                tile = pltpu.roll(jnp.where(straight, block, before), 0, 1, stride=1, stride_axis=0)
                toeplitz[j, :, c * 128:(c + 1) * 128] = tile.astype(BF16)

    each(0, 11, place)

    for k in order:
        values_to(k).wait()

    def unpack(step):
        for part in range(8):
            l = 8 * step + part
            x = got[l].astype(F32).reshape(16, 128)
            blocks[32 + l] = x.astype(BF16)
            blocks[l] = jnp.concatenate([jnp.zeros((2, 128), F32), x[:14]], axis=0).astype(BF16)

    each(0, 4, unpack)

    even = lax.rem(lax.broadcasted_iota(jnp.int32, (256, 128), 0), 2) == 0

    for side in range(2):
        def left(j):
            return blocks[32 - j + 16 * side:48 - j + 16 * side].reshape(256, 128)

        sums = jnp.dot(left(32), toeplitz[32], preferred_element_type=F32)
        for k in range(16):
            pair = jnp.concatenate([left(2 * k), left(2 * k + 1)], axis=1)
            sums += jnp.dot(pair, toeplitz[2 * k:2 * k + 2].reshape(256, 256), preferred_element_type=F32)
        chosen = jnp.where(even, sums[:, :128], sums[:, 128:])
        results[16 * side:16 * side + 16] = chosen.astype(BF16).reshape(16, 8, 2, 128)
    back_to(64).start()

    def far_first(step):
        for k in range(1, 4):
            back_to(64 + 3 * step + k).start()
            back_to(64 - 3 * step - k).start()

    each(0, 21, far_first)
    back[:, at, me] = results[pl.ds(16 * odd + 2 * at, 2), high]

    def near_first(step):
        for k in range(1, 4):
            back_to(3 * step + k).wait()
            back_to(128 - 3 * step - k).wait()

    each(0, 21, near_first)
    back_to(64).wait()


def mix_kernel(
    back, values_hbm, gates_hbm, skip_ref, weight_hbm, gathered, weight,
    values, gates, local_sem, right_send, left_recv, left_send, right_recv, on_send, on_recv,
):
    my_ch = lax.axis_index("ch")
    right, left, across = lax.rem(my_ch + 1, 4), lax.rem(my_ch + 3, 4), lax.rem(my_ch + 2, 4)
    barrier = pltpu.get_barrier_semaphore()
    for peer in (left, right):
        pl.semaphore_signal(barrier, inc=1, device_id={"ch": peer}, device_id_type=MESH)
    loads = [
        pltpu.make_async_copy(source, target, local_sem.at[k])
        for k, (source, target) in enumerate(((values_hbm, values), (gates_hbm, gates), (weight_hbm, weight)))
    ]
    for load in loads:
        load.start()
    loads[0].wait()
    loads[1].wait()
    wait_for(2)

    def piece(slot, quarter):
        return gathered.at[slot, pl.ds(64 * quarter, 64)]

    def to_right(quarter):
        return pltpu.make_async_remote_copy(
            src_ref=piece(my_ch, quarter), dst_ref=piece(my_ch, quarter), send_sem=right_send.at[quarter],
            recv_sem=left_recv.at[quarter], device_id={"ch": right}, device_id_type=MESH)

    def to_left(quarter):
        return pltpu.make_async_remote_copy(
            src_ref=piece(my_ch, quarter), dst_ref=piece(my_ch, quarter), send_sem=left_send.at[quarter],
            recv_sem=right_recv.at[quarter], device_id={"ch": left}, device_id_type=MESH)

    def pass_on(quarter):
        source, target = (left, right) if quarter < 2 else (right, left)
        return pltpu.make_async_remote_copy(
            src_ref=piece(source, quarter), dst_ref=piece(source, quarter), send_sem=on_send.at[quarter],
            recv_sem=on_recv.at[quarter], device_id={"ch": target}, device_id_type=MESH)

    for half in range(2):
        rows = slice(half * 128, (half + 1) * 128)
        arrived = back[half].astype(F32).reshape(256, 128)
        convolved = jnp.concatenate(
            [arrived[32 * w + 8 * q:32 * w + 8 * q + 8] for q in range(4) for w in range(NW)], axis=0).T
        hidden = (gates[rows, :] * (convolved + skip_ref[...] * values[rows, :])).astype(BF16)
        gathered[my_ch, rows, :] = hidden
        for quarter in (2 * half, 2 * half + 1):
            (to_left if half else to_right)(quarter).start()
    for quarter in (2, 3):
        to_right(quarter).start()
    for quarter in (0, 1):
        to_left(quarter).start()
    for first, second in ((0, 2), (1, 3)):
        to_right(first).wait_recv()
        pass_on(first).start()
        to_left(second).wait_recv()
        pass_on(second).start()
    loads[2].wait()
    for quarter in (2, 3):
        to_right(quarter).wait_recv()
    for quarter in (0, 1):
        to_left(quarter).wait_recv()
    for quarter in range(4):
        to_right(quarter).wait_send()
        to_left(quarter).wait_send()
        pass_on(quarter).wait()


def output_kernel(gathered, weight, out_hbm, out, out_sem):
    def store(half):
        rows = pl.ds(128 * half, 128)
        return pltpu.make_async_copy(out.at[rows], out_hbm.at[rows], out_sem.at[half])

    for half in range(2):
        rows = slice(128 * half, 128 * half + 128)
        for side in range(2):
            lanes = slice(256 * side, 256 * side + 256)
            sums = jnp.dot(gathered[0, rows, :], weight[0:256, lanes], preferred_element_type=F32)
            for k in range(1, 4):
                sums += jnp.dot(gathered[k, rows, :], weight[256 * k:256 * k + 256, lanes], preferred_element_type=F32)
            out[rows, lanes] = sums
        store(half).start()
    for half in range(2):
        store(half).wait()


def body(values, gates, filter_taps, skip, out_weight):
    dma = pltpu.SemaphoreType.DMA
    vmem = pl.BlockSpec(memory_space=VMEM)
    back = pl.pallas_call(
        convolve_kernel,
        out_shape=VMEM((2, NW, NZ, 2, 128), BF16),
        in_specs=[ANY, ANY],
        out_specs=vmem,
        scratch_shapes=[
            VMEM((256, 256), F32), VMEM((32, 256), F32), VMEM((2, NW, NZ, 2, 128), BF16),
            VMEM((NW, 8, 128), BF16), VMEM((NW, 8, 128), BF16), VMEM((18, NZ, 2, 128), BF16),
            VMEM((32, 8, 2, 128), BF16), VMEM((NZ, 2, 2, 128), BF16), VMEM((64, 16, 128), BF16),
            VMEM((68, 128), F32), VMEM((33, 128, 256), BF16), VMEM((32, 8, 2, 128), BF16),
            dma((2,)), dma((2, NW)), dma((2, NW)), dma((2, NZ)), dma((2, NZ)), dma((128,)), dma((128,)),
        ],
        compiler_params=pltpu.CompilerParams(collective_id=1, has_side_effects=True),
    )(values, filter_taps)
    near = lambda x: pltpu.with_memory_space_constraint(x, VMEM)
    gathered, weight = pl.pallas_call(
        mix_kernel,
        out_shape=(VMEM((4, 256, 256), BF16), VMEM((1024, 512), BF16)),
        in_specs=[vmem, ANY, ANY, vmem, ANY],
        out_specs=(vmem, vmem),
        scratch_shapes=[
            VMEM((256, 256), F32), VMEM((256, 256), F32),
            dma((3,)), dma((4,)), dma((4,)), dma((4,)), dma((4,)), dma((4,)), dma((4,)),
        ],
        compiler_params=pltpu.CompilerParams(collective_id=2, has_side_effects=True),
    )(near(back), values, gates, skip.reshape(1, 256), out_weight)
    return pl.pallas_call(
        output_kernel,
        out_shape=jax.ShapeDtypeStruct((256, 512), F32),
        in_specs=[vmem, vmem],
        out_specs=ANY,
        scratch_shapes=[VMEM((256, 512), F32), dma((2,))],
    )(near(gathered), near(weight))


def solution(mesh):
    torus = Mesh(mesh.devices.reshape(NZ, NW, 4), ("z", "w", "ch"))
    tokens = ("z", "w")
    return jax.shard_map(
        body,
        mesh=torus,
        in_specs=(P(tokens, "ch"), P(tokens, "ch"), P(tokens, "ch"), P("ch"), P(None, "ch")),
        out_specs=P(tokens, "ch"),
        check_vma=False,
    )
```

```python
import functools

import jax
import jax.numpy as jnp
from jax import lax
from jax.experimental import pallas as pl
from jax.experimental.pallas import tpu as pltpu
from jax.sharding import Mesh
from jax.sharding import PartitionSpec as P

MESH = pl.DeviceIdType.MESH
F32 = jnp.float32
BF16 = jnp.bfloat16
VMEM = pltpu.VMEM
ANY = pl.BlockSpec(memory_space=pl.ANY)
NZ, NW = 16, 8


def each(low, high, step):
    def run(k, _):
        step(k)
        return 0

    lax.fori_loop(low, high, run, 0)


def greet(axis, size):
    me = lax.axis_index(axis)
    barrier = pltpu.get_barrier_semaphore()
    for k in range(1, size):
        pl.semaphore_signal(barrier, inc=1, device_id={axis: lax.rem(me + k, size)}, device_id_type=MESH)


def wait_for(count):
    pl.semaphore_wait(pltpu.get_barrier_semaphore(), count)


def convolve_kernel(
    values_hbm, taps_hbm, back, values, taps, send_values, send_taps, near_taps, rows, got, got_taps, blocks, lags,
    toeplitz, results, local_sem, near_send, near_recv, send_sem, recv_sem, back_send, back_recv,
):
    at = lax.axis_index("w")
    me = lax.axis_index("z")
    greet("z", NZ)
    greet("w", NW)
    loads = [
        pltpu.make_async_copy(taps_hbm, taps, local_sem.at[0]),
        pltpu.make_async_copy(values_hbm, values, local_sem.at[1]),
    ]
    for load in loads:
        load.start()
    loads[0].wait()
    own = jnp.concatenate([taps[...], jnp.zeros((96, 256), F32)], axis=0)
    turned = own.T
    packed = turned[0:64] + pltpu.roll(turned[64:128], 32, 1)
    packed += pltpu.roll(turned[128:192], 64, 1) + pltpu.roll(turned[192:256], 96, 1)
    send_taps[...] = packed.astype(BF16).reshape(NW, 8, 128)
    loads[1].wait()
    for half in range(2):
        turned = values[half * 128:(half + 1) * 128, :].T
        for w in range(NW):
            own = jnp.concatenate([turned[64 * q + 8 * w:64 * q + 8 * w + 8] for q in range(4)], axis=0)
            send_values[half, w] = own.astype(BF16).reshape(NZ, 2, 128)
    wait_for(NW - 1 + NZ - 1)

    def taps_near(k):
        peer = lax.rem(at + k, NW)
        return pltpu.make_async_remote_copy(
            src_ref=send_taps.at[peer], dst_ref=near_taps.at[k], send_sem=near_send.at[0, k],
            recv_sem=near_recv.at[0, k], device_id={"w": peer}, device_id_type=MESH)

    def values_near(k):
        peer = lax.rem(at + k, NW)
        return pltpu.make_async_remote_copy(
            src_ref=send_values.at[:, peer], dst_ref=rows.at[pl.ds(2 * at, 2)], send_sem=near_send.at[1, k],
            recv_sem=near_recv.at[1, k], device_id={"w": peer}, device_id_type=MESH)

    near_order = (4, 3, 5, 2, 6, 1, 7)
    for k in near_order:
        taps_near(k).start()
        values_near(k).start()
    rows[pl.ds(2 * at, 2)] = send_values[:, at]
    near_taps[0] = send_taps[at]
    for k in near_order:
        taps_near(k).wait()
    lane = lax.broadcasted_iota(jnp.int32, (8, 128), 1)
    for half in range(2):
        parts = [near_taps[lax.rem(at + NW - w, NW)].astype(F32) for w in range(4 * half, 4 * half + 4)]
        lines = []
        for q in range(4):
            line = pltpu.roll(parts[3], 32 * ((3 - q) % 4), 1) if q != 3 else parts[3]
            for k in range(3):
                moved = pltpu.roll(parts[k], 32 * ((k - q) % 4), 1) if k != q else parts[k]
                line = jnp.where((lane >= 32 * k) & (lane < 32 * k + 32), moved, line)
            lines.append(line)
        rows[16 + half] = jnp.concatenate(lines, axis=0).astype(BF16).reshape(NZ, 2, 128)

    odd, high = lax.rem(me, 2), me // 2
    got_taps[me] = rows[16:18, me]

    def taps_to(k):
        peer = lax.rem(me + k, NZ)
        return pltpu.make_async_remote_copy(
            src_ref=rows.at[pl.ds(16, 2), peer], dst_ref=got_taps.at[me], send_sem=send_sem.at[0, k],
            recv_sem=recv_sem.at[0, k], device_id={"z": peer}, device_id_type=MESH)

    def values_to(k):
        peer = lax.rem(me + k, NZ)
        return pltpu.make_async_remote_copy(
            src_ref=rows.at[pl.ds(0, 16), peer], dst_ref=got.at[pl.ds(16 * odd, 16), high], send_sem=send_sem.at[1, k],
            recv_sem=recv_sem.at[1, k], device_id={"z": peer}, device_id_type=MESH)

    def back_to(k):
        peer = lax.rem(NW * me + at + k, NW * NZ)
        z, w = peer // NW, lax.rem(peer, NW)
        return pltpu.make_async_remote_copy(
            src_ref=results.at[pl.ds(16 * lax.rem(z, 2) + 2 * w, 2), z // 2], dst_ref=back.at[:, at, me],
            send_sem=back_send.at[k], recv_sem=back_recv.at[k], device_id={"z": z, "w": w}, device_id_type=MESH)

    order = (8, 7, 9, 6, 10, 5, 11, 4, 12, 3, 13, 2, 14, 1, 15)
    for k in order:
        taps_to(k).start()
    for k in near_order:
        values_near(k).wait()
    got[pl.ds(16 * odd, 16), high] = rows[0:16, me]
    for k in order:
        values_to(k).start()
    for k in order:
        taps_to(k).wait()
    lags[0:2] = jnp.zeros((2, 128), F32)
    lags[66:68] = jnp.zeros((2, 128), F32)
    for z in range(NZ):
        lags[2 + 4 * z:6 + 4 * z] = got_taps[z].astype(F32).reshape(4, 128)

    row = lax.broadcasted_iota(jnp.int32, (128, 128), 0)
    col = lax.broadcasted_iota(jnp.int32, (128, 128), 1)
    straight = col < 128 - row

    def place(step):
        for part in range(3):
            j = 3 * step + part
            for c in range(2):
                block = jnp.broadcast_to(lags[pl.ds(2 * j + 2 + c, 1), :], (128, 128))
                before = jnp.broadcast_to(lags[pl.ds(2 * j + c, 1), :], (128, 128))
                tile = pltpu.roll(jnp.where(straight, block, before), 0, 1, stride=1, stride_axis=0)
                toeplitz[j, :, c * 128:(c + 1) * 128] = tile.astype(BF16)

    each(0, 11, place)

    for k in order:
        values_to(k).wait()

    def unpack(step):
        for part in range(8):
            l = 8 * step + part
            x = got[l].astype(F32).reshape(16, 128)
            blocks[32 + l] = x.astype(BF16)
            blocks[l] = jnp.concatenate([jnp.zeros((2, 128), F32), x[:14]], axis=0).astype(BF16)

    each(0, 4, unpack)

    even = lax.rem(lax.broadcasted_iota(jnp.int32, (256, 128), 0), 2) == 0

    for side in range(2):
        def left(j):
            return blocks[32 - j + 16 * side:48 - j + 16 * side].reshape(256, 128)

        sums = jnp.dot(left(32), toeplitz[32], preferred_element_type=F32)
        for k in range(16):
            pair = jnp.concatenate([left(2 * k), left(2 * k + 1)], axis=1)
            sums += jnp.dot(pair, toeplitz[2 * k:2 * k + 2].reshape(256, 256), preferred_element_type=F32)
        chosen = jnp.where(even, sums[:, :128], sums[:, 128:])
        results[16 * side:16 * side + 16] = chosen.astype(BF16).reshape(16, 8, 2, 128)
    back_to(64).start()

    def far_first(step):
        for k in range(1, 4):
            back_to(64 + 3 * step + k).start()
            back_to(64 - 3 * step - k).start()

    each(0, 21, far_first)
    back[:, at, me] = results[pl.ds(16 * odd + 2 * at, 2), high]

    def near_first(step):
        for k in range(1, 4):
            back_to(3 * step + k).wait()
            back_to(128 - 3 * step - k).wait()

    each(0, 21, near_first)
    back_to(64).wait()


def mix_kernel(
    back, values_hbm, gates_hbm, skip_ref, weight_hbm, gathered, weight,
    values, gates, local_sem, right_send, left_recv, left_send, right_recv, on_send, on_recv,
):
    my_ch = lax.axis_index("ch")
    right, left, across = lax.rem(my_ch + 1, 4), lax.rem(my_ch + 3, 4), lax.rem(my_ch + 2, 4)
    barrier = pltpu.get_barrier_semaphore()
    for peer in (left, right):
        pl.semaphore_signal(barrier, inc=1, device_id={"ch": peer}, device_id_type=MESH)
    loads = [
        pltpu.make_async_copy(source, target, local_sem.at[k])
        for k, (source, target) in enumerate(((values_hbm, values), (gates_hbm, gates), (weight_hbm, weight)))
    ]
    for load in loads:
        load.start()
    loads[0].wait()
    loads[1].wait()

    def piece(slot, quarter):
        return gathered.at[slot, pl.ds(64 * quarter, 64)]

    def to_right(quarter):
        return pltpu.make_async_remote_copy(
            src_ref=piece(my_ch, quarter), dst_ref=piece(my_ch, quarter), send_sem=right_send.at[quarter],
            recv_sem=left_recv.at[quarter], device_id={"ch": right}, device_id_type=MESH)

    def to_left(quarter):
        return pltpu.make_async_remote_copy(
            src_ref=piece(my_ch, quarter), dst_ref=piece(my_ch, quarter), send_sem=left_send.at[quarter],
            recv_sem=right_recv.at[quarter], device_id={"ch": left}, device_id_type=MESH)

    def pass_on(quarter):
        source, target = (left, right) if quarter < 2 else (right, left)
        return pltpu.make_async_remote_copy(
            src_ref=piece(source, quarter), dst_ref=piece(source, quarter), send_sem=on_send.at[quarter],
            recv_sem=on_recv.at[quarter], device_id={"ch": target}, device_id_type=MESH)

    for half in range(2):
        rows = slice(half * 128, (half + 1) * 128)
        arrived = back[half].astype(F32).reshape(256, 128)
        convolved = jnp.concatenate(
            [arrived[32 * w + 8 * q:32 * w + 8 * q + 8] for q in range(4) for w in range(NW)], axis=0).T
        hidden = (gates[rows, :] * (convolved + skip_ref[...] * values[rows, :])).astype(BF16)
        gathered[my_ch, rows, :] = hidden
    wait_for(2)
    for right_one, left_one in ((0, 2), (1, 3), (2, 0), (3, 1)):
        to_right(right_one).start()
        to_left(left_one).start()
    for first, second in ((0, 2), (1, 3)):
        to_right(first).wait_recv()
        pass_on(first).start()
        to_left(second).wait_recv()
        pass_on(second).start()
    loads[2].wait()
    for quarter in (2, 3):
        to_right(quarter).wait_recv()
    for quarter in (0, 1):
        to_left(quarter).wait_recv()
    for quarter in range(4):
        to_right(quarter).wait_send()
        to_left(quarter).wait_send()
        pass_on(quarter).wait()


def output_kernel(gathered, weight, out_hbm, out, out_sem):
    def store(half):
        rows = pl.ds(128 * half, 128)
        return pltpu.make_async_copy(out.at[rows], out_hbm.at[rows], out_sem.at[half])

    for half in range(2):
        rows = slice(128 * half, 128 * half + 128)
        for side in range(2):
            lanes = slice(256 * side, 256 * side + 256)
            sums = jnp.dot(gathered[0, rows, :], weight[0:256, lanes], preferred_element_type=F32)
            for k in range(1, 4):
                sums += jnp.dot(gathered[k, rows, :], weight[256 * k:256 * k + 256, lanes], preferred_element_type=F32)
            out[rows, lanes] = sums
        store(half).start()
    for half in range(2):
        store(half).wait()


def body(values, gates, filter_taps, skip, out_weight):
    dma = pltpu.SemaphoreType.DMA
    vmem = pl.BlockSpec(memory_space=VMEM)
    back = pl.pallas_call(
        convolve_kernel,
        out_shape=VMEM((2, NW, NZ, 2, 128), BF16),
        in_specs=[ANY, ANY],
        out_specs=vmem,
        scratch_shapes=[
            VMEM((256, 256), F32), VMEM((32, 256), F32), VMEM((2, NW, NZ, 2, 128), BF16),
            VMEM((NW, 8, 128), BF16), VMEM((NW, 8, 128), BF16), VMEM((18, NZ, 2, 128), BF16),
            VMEM((32, 8, 2, 128), BF16), VMEM((NZ, 2, 2, 128), BF16), VMEM((64, 16, 128), BF16),
            VMEM((68, 128), F32), VMEM((33, 128, 256), BF16), VMEM((32, 8, 2, 128), BF16),
            dma((2,)), dma((2, NW)), dma((2, NW)), dma((2, NZ)), dma((2, NZ)), dma((128,)), dma((128,)),
        ],
        compiler_params=pltpu.CompilerParams(collective_id=1, has_side_effects=True),
    )(values, filter_taps)
    near = lambda x: pltpu.with_memory_space_constraint(x, VMEM)
    gathered, weight = pl.pallas_call(
        mix_kernel,
        out_shape=(VMEM((4, 256, 256), BF16), VMEM((1024, 512), BF16)),
        in_specs=[vmem, ANY, ANY, vmem, ANY],
        out_specs=(vmem, vmem),
        scratch_shapes=[
            VMEM((256, 256), F32), VMEM((256, 256), F32),
            dma((3,)), dma((4,)), dma((4,)), dma((4,)), dma((4,)), dma((4,)), dma((4,)),
        ],
        compiler_params=pltpu.CompilerParams(collective_id=2, has_side_effects=True),
    )(near(back), values, gates, skip.reshape(1, 256), out_weight)
    return pl.pallas_call(
        output_kernel,
        out_shape=jax.ShapeDtypeStruct((256, 512), F32),
        in_specs=[vmem, vmem],
        out_specs=ANY,
        scratch_shapes=[VMEM((256, 512), F32), dma((2,))],
    )(near(gathered), near(weight))


def solution(mesh):
    torus = Mesh(mesh.devices.reshape(NZ, NW, 4), ("z", "w", "ch"))
    tokens = ("z", "w")
    return jax.shard_map(
        body,
        mesh=torus,
        in_specs=(P(tokens, "ch"), P(tokens, "ch"), P(tokens, "ch"), P("ch"), P(None, "ch")),
        out_specs=P(tokens, "ch"),
        check_vma=False,
    )
```
